256 devices in a mesh: leaf: 32 (over y, x, core), row: 8 (over z).
Axes of the slice: x: 4, y: 4, z: 8, core: 2. Of those that a mesh axis runs over, the one named last changes fastest.
Arguments:
- sources_root: float32 [64, 32, 128], P('leaf'), may hold values from -6 to 6
- sources_upper: float32 [64, 32, 128], P('leaf'), may hold values from -6 to 6
- sources_middle: float32 [64, 32, 128], P('leaf'), may hold values from -6 to 6
- sources_lower: float32 [64, 32, 128], P('leaf'), may hold values from -6 to 6
- inverse_root: float32 [64, 128, 8192], P('leaf', None, 'row'), may hold values from -4 to 4, as said below
- inverse_upper: float32 [64, 128, 4096], P('leaf', None, 'row'), may hold values from -4 to 4, as said below
- inverse_middle: float32 [64, 128, 2048], P('leaf', None, 'row'), may hold values from -4 to 4, as said below
- inverse_lower: float32 [64, 128, 1024], P('leaf', None, 'row'), may hold values from -4 to 4, as said below
- update_upper: float32 [128, 128, 4096], P('leaf', None, 'row'), may hold values from -0.046875 to 0.046875
- update_middle: float32 [256, 128, 2048], P('leaf', None, 'row'), may hold values from -0.0625 to 0.0625
- update_lower: float32 [256, 128, 1024], P('leaf', None, 'row'), may hold values from -0.09375 to 0.09375
- links_upper: int32 [128], P('leaf'), may hold values from 0 to 63, as said below
- links_middle: int32 [256], P('leaf'), may hold values from 0 to 127, as said below
- links_lower: int32 [256], P('leaf'), may hold values from 0 to 191, as said below
Outputs:
- adjoint_root: float32 [64, 32, 128], P('leaf')
- adjoint_upper: float32 [64, 32, 128], P('leaf')
- adjoint_middle: float32 [64, 32, 128], P('leaf')
- adjoint_lower: float32 [64, 32, 128], P('leaf')
The draws below stay inside these ranges and needn't reach their ends.
Inputs may be any that keep to these rules, and one draw needn't show every extreme that they name: `inverse_root`: lower triangular: stored entry [g, t, p] is zero where g * 128 + t > p. `inverse_upper`: lower triangular: stored entry [g, t, p] is zero where (g % 32) * 128 + t > p. `inverse_middle`: lower triangular: stored entry [g, t, p] is zero where (g % 16) * 128 + t > p. `inverse_lower`: lower triangular: stored entry [g, t, p] is zero where (g % 8) * 128 + t > p. `links_upper`: the entries of one front are distinct and all belong to the root front. `links_middle`: the entries of one front are distinct and belong to the front's own ancestors (the root and its parent of level 1). `links_lower`: the entries of one front are distinct and belong to the front's own ancestors on levels 0 to 2.
All inputs are finite; a program needn't handle non-finite values.
Results may differ from the reference program's by a relative error of at most 0.00014.
Values sent between devices are 32-bit elements; how exact they have to be, the bound alone decides.
No kernel may reach another device: no remote copies, remote signals or barrier semaphores. Data moves between devices by JAX's collectives and lax.ppermute only.
A program may use at most 64 MiB of HBM per device.

```python
import math
import jax
import jax.numpy as jnp
from jax import lax

PIV_ROOT = 8192
BLOCK_ROWS = 128
RESIDUALS = 32
PIV_UPPER = 4096
PIV_MIDDLE = 2048
PIV_LOWER = 1024
UPD_UPPER = 8192
UPD_MIDDLE = 8192
UPD_LOWER = 4096


def make_inverse(base_key, fronts, pivots):
    shape = (fronts, pivots // BLOCK_ROWS, BLOCK_ROWS, pivots)
    column = lax.broadcasted_iota(jnp.int32, shape, 1) * BLOCK_ROWS + lax.broadcasted_iota(jnp.int32, shape, 2)
    row_index = lax.broadcasted_iota(jnp.int32, shape, 3)
    first, second = jax.random.split(base_key, 2)
    beside = jax.random.normal(first, shape, jnp.float32) * (0.5 / math.sqrt(pivots))
    diagonal = jax.random.uniform(second, shape, jnp.float32, 0.8, 1.6)
    values = jnp.where(column == row_index, diagonal, jnp.where(column < row_index, beside, 0.0))
    return values.astype(jnp.float32).reshape(fronts * (pivots // BLOCK_ROWS), BLOCK_ROWS, pivots)


def make_links(base_key, level_in_tree, fronts, amount):
    blocks = PIV_ROOT // BLOCK_ROWS

    def single(front_key, front):
        pieces = []
        for upper_level in range(level_in_tree):
            across = (PIV_ROOT >> upper_level) // BLOCK_ROWS
            owner = jnp.right_shift(front, level_in_tree - upper_level)
            pieces.append(upper_level * blocks + owner * across + jnp.arange(across, dtype=jnp.int32))
        candidates = jnp.concatenate(pieces)
        shuffled = jax.random.permutation(front_key, candidates.shape[0])
        return candidates[shuffled[:amount]].astype(jnp.int32)
    front_keys = jax.random.split(base_key, fronts)
    return jax.vmap(single)(front_keys, jnp.arange(fronts, dtype=jnp.int32)).reshape(-1)


def draw_inverse_root(key, part):
    return make_inverse(jax.random.fold_in(key, 101), 1, PIV_ROOT)


def draw_inverse_upper(key, part):
    return make_inverse(jax.random.fold_in(key, 102), 2, PIV_UPPER)


def draw_inverse_middle(key, part):
    return make_inverse(jax.random.fold_in(key, 103), 4, PIV_MIDDLE)


def draw_inverse_lower(key, part):
    return make_inverse(jax.random.fold_in(key, 104), 8, PIV_LOWER)


def draw_links_upper(key, part):
    return make_links(jax.random.fold_in(key, 201), 1, 2, UPD_UPPER // BLOCK_ROWS)


def draw_links_middle(key, part):
    return make_links(jax.random.fold_in(key, 202), 2, 4, UPD_MIDDLE // BLOCK_ROWS)


def draw_links_lower(key, part):
    return make_links(jax.random.fold_in(key, 203), 3, 8, UPD_LOWER // BLOCK_ROWS)


def shard_levels(key, extent, cuts, smallest, high):
    level = 1.0
    for axis_at, parts in cuts:
        heights = jax.random.uniform(jax.random.fold_in(jax.random.fold_in(key, 6), axis_at), (parts,), jnp.float32, smallest / len(cuts), high / len(cuts))
        level = level * jnp.repeat(jnp.exp(heights), extent[axis_at] // parts).reshape((-1,) + (1,) * (len(extent) - 1 - axis_at))
    return level


def noise(own_key, dims, width, reach, cuts=(), held_as=jnp.bfloat16):
    loudness = shard_levels(own_key, dims, cuts, -0.22, 0.18) if cuts else 1.0
    values = jax.random.normal(own_key, dims, jnp.float32) * width * loudness
    return jnp.minimum(jnp.maximum(values, -reach), reach).astype(held_as)


def setup_inputs(seed: int = 0) -> dict:
    keys = jax.random.split(jax.random.key(seed), 15)
    return {
        "sources_root": noise(keys[0], (PIV_ROOT // BLOCK_ROWS, RESIDUALS, BLOCK_ROWS), 1.0, 6.0, ((0, 32),), jnp.float32),
        "sources_upper": noise(keys[1], (PIV_ROOT // BLOCK_ROWS, RESIDUALS, BLOCK_ROWS), 1.0, 6.0, ((0, 32),), jnp.float32),
        "sources_middle": noise(keys[2], (PIV_ROOT // BLOCK_ROWS, RESIDUALS, BLOCK_ROWS), 1.0, 6.0, ((0, 32),), jnp.float32),
        "sources_lower": noise(keys[3], (PIV_ROOT // BLOCK_ROWS, RESIDUALS, BLOCK_ROWS), 1.0, 6.0, ((0, 32),), jnp.float32),
        "inverse_root": draw_inverse_root(jax.random.fold_in(keys[14], 71), 0),
        "inverse_upper": draw_inverse_upper(jax.random.fold_in(keys[14], 71), 0),
        "inverse_middle": draw_inverse_middle(jax.random.fold_in(keys[14], 71), 0),
        "inverse_lower": draw_inverse_lower(jax.random.fold_in(keys[14], 71), 0),
        "update_upper": noise(keys[8], (2 * UPD_UPPER // BLOCK_ROWS, BLOCK_ROWS, PIV_UPPER), (4 * PIV_UPPER) ** -0.5, 0.046875, ((0, 32), (2, 8)), jnp.float32),
        "update_middle": noise(keys[9], (4 * UPD_MIDDLE // BLOCK_ROWS, BLOCK_ROWS, PIV_MIDDLE), (4 * PIV_MIDDLE) ** -0.5, 0.0625, ((0, 32), (2, 8)), jnp.float32),
        "update_lower": noise(keys[10], (8 * UPD_LOWER // BLOCK_ROWS, BLOCK_ROWS, PIV_LOWER), (4 * PIV_LOWER) ** -0.5, 0.09375, ((0, 32), (2, 8)), jnp.float32),
        "links_upper": draw_links_upper(jax.random.fold_in(keys[14], 71), 0),
        "links_middle": draw_links_middle(jax.random.fold_in(keys[14], 71), 0),
        "links_lower": draw_links_lower(jax.random.fold_in(keys[14], 71), 0),
    }


def reference(sources_root, sources_upper, sources_middle, sources_lower, inverse_root, inverse_upper, inverse_middle, inverse_lower, update_upper, update_middle, update_lower, links_upper, links_middle, links_lower):
    highest = lax.Precision.HIGHEST
    blocks = PIV_ROOT // BLOCK_ROWS
    pivots = [PIV_ROOT, PIV_UPPER, PIV_MIDDLE, PIV_LOWER]
    uppers = [0, UPD_UPPER, UPD_MIDDLE, UPD_LOWER]
    raw_sources = [sources_root, sources_upper, sources_middle, sources_lower]
    raw_inverse = [inverse_root, inverse_upper, inverse_middle, inverse_lower]
    raw_update = [None, update_upper, update_middle, update_lower]
    raw_links = [None, links_upper, links_middle, links_lower]
    sources = [raw_sources[level].reshape(1 << level, pivots[level] // BLOCK_ROWS, RESIDUALS, BLOCK_ROWS) for level in range(4)]
    inverse_factor = [raw_inverse[level].reshape(1 << level, pivots[level] // BLOCK_ROWS, BLOCK_ROWS, pivots[level]) for level in range(4)]
    update = [None] + [raw_update[level].reshape(1 << level, uppers[level] // BLOCK_ROWS, BLOCK_ROWS, pivots[level]) for level in range(1, 4)]
    links = [None] + [raw_links[level].reshape(1 << level, uppers[level] // BLOCK_ROWS) for level in range(1, 4)]
    pending = [jnp.zeros((blocks, RESIDUALS, BLOCK_ROWS), jnp.float32) for level_in_tree in range(4)]
    forward = [None, None, None, None]
    for level_in_tree in (3, 2, 1, 0):
        source_vector = sources[level_in_tree] - pending[level_in_tree].reshape(sources[level_in_tree].shape)
        solved = jnp.einsum("fbtp,fbrt->frp", inverse_factor[level_in_tree], source_vector, precision=highest)
        forward[level_in_tree] = solved
        if level_in_tree > 0:
            matrix_product = jnp.einsum("fktp,frp->fkrt", update[level_in_tree], solved, precision=highest)
            stacked_terms = matrix_product.reshape(-1, RESIDUALS, BLOCK_ROWS)
            target = links[level_in_tree].reshape(-1).astype(jnp.int32)
            spread = jnp.zeros((level_in_tree * blocks, RESIDUALS, BLOCK_ROWS), jnp.float32).at[target].add(stacked_terms)
            for upper_level in range(level_in_tree):
                pending[upper_level] = pending[upper_level] + spread[upper_level * blocks:(upper_level + 1) * blocks]
    solutions = [None, None, None, None]
    for level_in_tree in range(4):
        fixed_update = forward[level_in_tree]
        if level_in_tree > 0:
            stacked = jnp.concatenate([solutions[upper_level].reshape(blocks, RESIDUALS, BLOCK_ROWS) for upper_level in range(level_in_tree)], axis=0)
            picked = stacked[links[level_in_tree].astype(jnp.int32)]
            backward = jnp.einsum("fktp,fkrt->frp", update[level_in_tree], picked, precision=highest)
            fixed_update = fixed_update - backward
        solutions[level_in_tree] = jnp.einsum("fbtp,frp->fbrt", inverse_factor[level_in_tree], fixed_update, precision=highest)
    outputs = [solutions[level].reshape(blocks, RESIDUALS, BLOCK_ROWS) for level in range(4)]
    return (outputs[0], outputs[1], outputs[2], outputs[3])
```

```python
import jax
import jax.numpy as jnp
from jax import lax
from jax.sharding import Mesh, PartitionSpec as P


BLOCKS = 64
PREC = lax.Precision.HIGH
AXES = ("yh", "yl", "xh", "xl", "core", "row")
LEAF = AXES[:5]
CHIPS = [("yh", "yl", "xh", "xl"), ("yl", "xh", "xl"), ("xh", "xl"), ("xl",)]


def size_of(axes):
    total = 1
    for axis in axes:
        total *= lax.axis_size(axis)
    return total


def exchange(pieces, axes):
    return lax.all_to_all(pieces, axes, split_axis=0, concat_axis=0, tiled=True)


def gathered(x, axes):
    return exchange(jnp.broadcast_to(x, (size_of(axes), *x.shape)), axes)


def total_over(x, axes):
    return gathered(x, axes).sum(axis=0)


def swapped(x, axis):
    return lax.ppermute(x, axis, [(0, 1), (1, 0)])


def leaf_total(x, level):
    axes = CHIPS[level]
    if level == 3:
        return x + swapped(x, "xl")
    if level == 2:
        x = x + swapped(x, "xl")
        return x + swapped(x, "xh")
    if level == 1:
        return total_over(x, axes)
    x = total_over(x, ("xh", "xl"))
    return total_over(x, ("yh", "yl"))


def body(*args):
    sources, inverse = args[0:4], args[4:8]
    update = [None, *args[8:11]]
    links = [None, *args[11:14]]
    core = lax.axis_index("core")
    first = core == 0
    half = sources[0].shape[1] // 2

    both = jnp.stack(sources)
    low, high = both[:, :, :half], both[:, :, half:]
    kept = jnp.where(first, low, high)
    handed = swapped(jnp.where(first, high, low), "core")
    own = [kept[level] for level in range(4)]
    other = [handed[level] for level in range(4)]
    inverse_other, update_other, links_all = [None] * 4, [None] * 4, [None] * 4
    for level in (3, 2, 1, 0):
        inverse_other[level] = swapped(inverse[level], "core")
        if level:
            update_other[level] = swapped(update[level], "core")
            links_all[level] = jnp.concatenate(
                [links[level], swapped(links[level], "core")]
            )

    def in_order(mine, theirs):
        return jnp.where(
            first,
            jnp.concatenate([mine, theirs], axis=0),
            jnp.concatenate([theirs, mine], axis=0),
        )

    counts = [BLOCKS >> level for level in range(4)]
    pending = [None] * 3
    picks = [None] * 4
    forward = [None] * 4
    for level in (3, 2, 1, 0):
        mine, theirs = own[level], other[level]
        if level < 3:
            pieces = pending[level]
            axes = CHIPS[level]
            pieces = pieces.reshape(size_of(axes), 4, *pieces.shape[1:])
            arrived = total_over(exchange(pieces, axes).sum(axis=0), ("row",))
            mine = mine - jnp.where(first, arrived[:2], arrived[2:])
            theirs = theirs - jnp.where(first, arrived[2:], arrived[:2])
        partial = jnp.einsum(
            "dkx,dek->ex", inverse[level], mine, precision=PREC
        ) + jnp.einsum("dkx,dek->ex", inverse_other[level], theirs, precision=PREC)
        solved = leaf_total(partial, level)
        forward[level] = solved
        if level:
            product = jnp.concatenate(
                [
                    jnp.einsum("ktp,rp->krt", update[level], solved, precision=PREC),
                    jnp.einsum(
                        "ktp,rp->krt", update_other[level], solved, precision=PREC
                    ),
                ],
                axis=0,
            )
            level_of = links_all[level] // BLOCKS
            picks[level] = []
            for upper in range(level):
                within = links_all[level] % counts[upper]
                hits = (level_of == upper)[:, None] & (
                    within[:, None] == jnp.arange(counts[upper], dtype=jnp.int32)[None]
                )
                hits = hits.astype(jnp.float32)
                picks[level].append(hits)
                spread = jnp.einsum("xs,xon->son", hits, product, precision=PREC)
                pending[upper] = (
                    spread if pending[upper] is None else pending[upper] + spread
                )
    outputs = []
    fronts = []
    for level in range(4):
        reduced = forward[level]
        if level:
            picked = sum(
                jnp.einsum("wq,qfx->wfx", picks[level][upper], fronts[upper], precision=PREC)
                for upper in range(level)
            )
            n = update[level].shape[0]
            partial = jnp.einsum(
                "ktp,krt->rp", update[level], picked[:n], precision=PREC
            ) + jnp.einsum("ktp,krt->rp", update_other[level], picked[n:], precision=PREC)
            reduced = reduced - leaf_total(partial, level)
        solution_mine = jnp.einsum("hay,zy->hza", inverse[level], reduced, precision=PREC)
        solution_theirs = jnp.einsum(
            "hay,zy->hza", inverse_other[level], reduced, precision=PREC
        )
        solved = total_over(in_order(solution_mine, solution_theirs), ("row",))
        if level < 3:
            whole = gathered(solved, CHIPS[level])
            fronts.append(whole.reshape(-1, *whole.shape[2:]))
        mine = jnp.where(first, solved[:2], solved[2:])
        theirs = swapped(jnp.where(first, solved[2:], solved[:2]), "core")
        outputs.append(
            jnp.where(
                first,
                jnp.concatenate([mine, theirs], axis=1),
                jnp.concatenate([theirs, mine], axis=1),
            )
        )
    return tuple(outputs)


def solution(mesh):
    fine = Mesh(mesh.devices.reshape(2, 2, 2, 2, 2, 8), AXES)
    vector, matrix, index = P(LEAF, None, None), P(LEAF, None, "row"), P(LEAF)
    return jax.shard_map(
        body,
        mesh=fine,
        in_specs=(vector,) * 4 + (matrix,) * 7 + (index,) * 3,
        out_specs=(vector,) * 4,
        check_vma=False,
    )
```

```python
import functools

import jax
import jax.numpy as jnp
from jax import lax
from jax.experimental import pallas as pl
from jax.experimental.pallas import tpu as pltpu
from jax.sharding import Mesh, PartitionSpec as P


AXES = ("yh", "yl", "xh", "xl", "core", "row")
LEAF = AXES[:5]
X4 = ("xh", "xl")
ALL_X = ("yl", "xh", "xl")
TOP = ("yh", "xh", "xl")
F32 = jnp.float32


def size_of(axes):
    total = 1
    for axis in axes:
        total *= lax.axis_size(axis)
    return total


def exchange(pieces, axes):
    return lax.all_to_all(pieces, axes, split_axis=0, concat_axis=0, tiled=True)


def swapped(x, axis):
    return lax.ppermute(x, axis, [(0, 1), (1, 0)])


def halves(x):
    high = x.astype(jnp.bfloat16)
    return high, (x - high.astype(F32)).astype(jnp.bfloat16)


def doubled(a):
    high = a.astype(jnp.bfloat16).astype(F32)
    return jnp.concatenate([high, a - high], axis=0).astype(jnp.bfloat16)


def product(rows, matrix, transposed):
    r = rows.shape[0]
    pair = doubled(rows)
    high, low = halves(matrix)
    dims = (((1,), (1 if transposed else 0,)), ((), ()))
    both = lax.dot_general(pair, high, dims, preferred_element_type=F32)
    both = both + lax.dot_general(pair, low, dims, preferred_element_type=F32)
    return both[:r] + both[r:]


def summed(ref, *index):
    total = ref[(0, *index)]
    for i in range(1, ref.shape[0]):
        total = total + ref[(i, *index)]
    return total


def call(kernel, outs, scalars, arrays, scratch=(), flops=2_000_000):
    size = sum(a.size for a in arrays) * 4
    single = isinstance(outs, tuple)
    shapes = [outs] if single else list(outs)
    result = pl.pallas_call(
        kernel,
        out_shape=[jax.ShapeDtypeStruct(s, F32) for s in shapes],
        in_specs=[pl.BlockSpec(memory_space=pltpu.SMEM)] * len(scalars)
        + [pl.BlockSpec(memory_space=pltpu.VMEM)] * len(arrays),
        out_specs=[pl.BlockSpec(memory_space=pltpu.VMEM)] * len(shapes),
        scratch_shapes=list(scratch),
        cost_estimate=pl.CostEstimate(
            flops=flops, bytes_accessed=size, transcendentals=0
        ),
    )(*scalars, *arrays)
    return result[0] if single else result


def value_kernel(copies, arrives, slots, *refs):
    refs = list(refs)
    arrived = refs.pop(0) if arrives else None
    sources, inverses, out = refs[:copies], refs[copies : 2 * copies], refs[2 * copies]
    total = None
    for k in range(copies):
        rows = []
        for b in range(2):
            w = sources[k][b]
            if arrives:
                w = w - summed(arrived, slots[k] * 2 + b)
            rows.append(w)
        width = inverses[k].shape[2]
        part = product(
            jnp.concatenate(rows, axis=1), inverses[k][...].reshape(256, width), False
        )
        total = part if total is None else total + part
    for i in range(out.shape[0]):
        out[i] = total


def contributions(solved, updates, add):
    j = 0
    for update in updates:
        for start in range(0, update.shape[0], 2):
            both = product(
                solved, update[start : start + 2].reshape(256, update.shape[2]), True
            )
            add(j, both[:, :128])
            add(j + 1, both[:, 128:])
            j += 2


def push_wide_kernel(level, places, *refs):
    if level == 3:
        pieces, refs = refs[:2], refs[2:]
        solved = pieces[0][...] + pieces[1][...]
        updates, (solved_ref, out2, out1, out0, dense) = refs[:2], refs[2:]
    else:
        pieces, old1, old0, refs = refs[0], refs[1], refs[2], refs[3:]
        solved = summed(pieces)
        updates, (solved_ref, out1, out0, dense) = refs[:2], refs[2:]
    solved_ref[...] = solved
    if level == 3:
        dense[...] = jnp.zeros(dense.shape, F32)
    else:
        dense[:, 16:48] = old1[...].reshape(2, 32, 8, 128)
        dense[:, 48:112] = old0[...]

    def add(j, block):
        place = places[j]
        dense[0, place] += block[:8]
        dense[1, place] += block[8:]

    contributions(solved, updates, add)
    if level == 3:
        out2[:, :8] = dense[0, 0:16]
        out2[:, 8:] = dense[1, 0:16]
    out1[...] = dense[:, 16:48].reshape(out1.shape)
    out0[...] = dense[:, 48:112]


def push_top_kernel(side, places, *refs):
    pieces, old0, extra0, refs = refs[0], refs[1], refs[2], refs[3:]
    updates, (solved_ref, dense) = refs[:4], refs[4:]
    solved = summed(pieces)
    solved_ref[...] = solved
    dense[...] = old0[side[0]] + extra0[...]

    def add(j, block):
        dense[places[j]] += block

    contributions(solved, updates, add)


def copies_kernel(pieces, out):
    total = summed(pieces)
    for i in range(out.shape[0]):
        out[i] = total


def share_kernel(pieces, solved, out):
    total = summed(pieces)
    solved[...] = total
    for i in range(out.shape[0]):
        out[i] = total


def solution_kernel(copies, minus, slots, *refs):
    if minus == 0:
        refs, z = refs[1:], summed(refs[0])
    elif minus == 1:
        refs, z = refs[2:], refs[0][...] - summed(refs[1])
    else:
        refs, z = refs[3:], refs[0][...] - (refs[1][...] + refs[2][...])
    inverses, out = refs[:copies], refs[copies]
    for k in range(copies):
        both = product(z, inverses[k][...].reshape(256, inverses[k].shape[2]), True)
        for i in range(out.shape[0]):
            out[i, slots[k] * 2] = both[:, :128]
            out[i, slots[k] * 2 + 1] = both[:, 128:]


def products_of(pick, updates):
    total, j = None, 0
    for update in updates:
        for start in range(0, update.shape[0], 2):
            rows = jnp.concatenate([pick(j), pick(j + 1)], axis=1)
            part = product(
                rows, update[start : start + 2].reshape(256, update.shape[2]), False
            )
            total = part if total is None else total + part
            j += 2
    return total


def pull_top_kernel(places, front, *refs):
    updates, out = refs[:4], refs[4]
    total = products_of(lambda j: front[places[j]], updates)
    for i in range(out.shape[0]):
        out[i] = total


def pull_wide_kernel(level, side, places, own0, other0, front1, *refs):
    if level == 3:
        front2, refs = refs[0], refs[1:]
    updates, (out, dense) = refs[:2], refs[2:]
    dense[side[0], 48:112] = own0[...]
    dense[1 - side[0], 48:112] = other0[...]
    dense[:, 16:48] = front1[...].reshape(2, 32, 8, 128)
    if level == 3:
        dense[0, 0:16] = front2[:, :8]
        dense[1, 0:16] = front2[:, 8:]
    total = products_of(
        lambda j: jnp.concatenate([dense[0, places[j]], dense[1, places[j]]], axis=0),
        updates,
    )
    if level == 3:
        out[...] = total
    else:
        for i in range(out.shape[0]):
            out[i] = total


def last_kernel(slots, pieces, kept, handed):
    for b in range(2):
        kept[b] = summed(pieces, slots[0] * 2 + b)
        handed[b] = summed(pieces, slots[1] * 2 + b)


def merge_kernel(side, kept, handed, out):
    out[:, pl.ds(pl.multiple_of(side[0] * 16, 16), 16)] = kept[...]
    out[:, pl.ds(pl.multiple_of((1 - side[0]) * 16, 16), 16)] = handed[...]


def place_of(link):
    def permuted(g):
        return (g & 32) | (((g >> 2) & 3) << 3) | (((g >> 4) & 1) << 2) | (g & 3)

    level = link >> 6
    return jnp.where(
        level == 0,
        48 + permuted(link & 63),
        jnp.where(level == 1, 16 + permuted(link & 31), link & 15),
    )


def body(*args):
    sources, inverse = args[0:4], args[4:8]
    update, links = [None, *args[8:11]], [None, *args[11:14]]
    core, side = lax.axis_index("core"), lax.axis_index("yl")
    first, lower = core == 0, side == 0
    half, quarter = 16, 8

    def where_half(x, test, size, axis):
        a = lax.slice_in_dim(x, 0, size, axis=axis)
        b = lax.slice_in_dim(x, size, 2 * size, axis=axis)
        return jnp.where(test, a, b), jnp.where(test, b, a)

    deep, deep_given = where_half(jnp.stack(sources[2:]), first, half, 2)
    deep_other = swapped(deep_given, "core")
    inverses = [None] * 4
    inverses[3] = [inverse[3], swapped(inverse[3], "core")]
    updates = [None] * 4
    updates[3] = [update[3], swapped(update[3], "core")]
    inverses[2] = [inverse[2], swapped(inverse[2], "core")]
    updates[2] = [update[2], swapped(update[2], "core")]
    across = {}
    across["i1"] = swapped(inverse[1], "yl")
    across["u1"] = swapped(update[1], "yl")
    across["i0"] = swapped(inverse[0], "yl")
    inverses[1] = [inverse[1], swapped(inverse[1], "core"), across["i1"], swapped(across["i1"], "core")]
    updates[1] = [update[1], swapped(update[1], "core"), across["u1"], swapped(across["u1"], "core")]
    inverses[0] = [inverse[0], swapped(inverse[0], "core"), across["i0"], swapped(across["i0"], "core")]

    top, top_given = where_half(jnp.stack(sources[:2]), first, half, 2)
    top_other = swapped(top_given, "core")
    quad, quad_given = where_half(jnp.stack([top, top_other]), lower, quarter, 3)
    quad_far = swapped(quad_given, "yl")
    source_of = [
        [quad[0, 0], quad[1, 0], quad_far[0, 0], quad_far[1, 0]],
        [quad[0, 1], quad[1, 1], quad_far[0, 1], quad_far[1, 1]],
        [deep[0], deep_other[0]],
        [deep[1], deep_other[1]],
    ]

    place = [None] * 4
    all_links = jnp.concatenate([place_of(links[1]), place_of(links[2]), place_of(links[3])])
    core_links = swapped(all_links, "core")
    far_links = swapped(jnp.stack([links[1], core_links[:4]]), "yl")
    place[3] = jnp.concatenate([all_links[12:20], core_links[12:20]])
    place[2] = jnp.concatenate([all_links[4:12], core_links[4:12]])
    place[1] = (
        jnp.concatenate([all_links[:4], core_links[:4], place_of(far_links[0]), far_links[1]]) - 48
    )

    slots_wide = jnp.stack([core, 1 - core]).astype(jnp.int32)
    slots_top = jnp.concatenate([side * 2 + slots_wide, (1 - side) * 2 + slots_wide]).astype(jnp.int32)
    side1 = side.astype(jnp.int32).reshape(1)
    core1 = core.astype(jnp.int32).reshape(1)
    slots = [slots_top, slots_top, slots_wide, slots_wide]
    copies = [4, 4, 2, 2]
    widths = [i.shape[2] for i in inverse]

    def value(level, arrived, n):
        rows = 8 if level < 2 else 16
        lead = [] if arrived is None else [arrived]
        return call(
            functools.partial(value_kernel, copies[level], arrived is not None),
            (n, rows, widths[level]),
            [slots[level]],
            [*lead, *source_of[level], *inverses[level]],
        )

    def row_copies(pieces, axes):
        pieces = exchange(pieces, axes)
        n = pieces.shape[0]
        out = call(copies_kernel, (8, *pieces.shape[1:]), [], [pieces])
        return exchange(out, ("row",))

    dense_scratch = [pltpu.VMEM((2, 112, 8, 128), F32)]
    part3 = value(3, None, 1)[0]
    y3, d2, d1, d0 = call(
        functools.partial(push_wide_kernel, 3),
        [(16, widths[3]), (16, 16, 128), (8, 8, 8, 128), (2, 64, 8, 128)],
        [place[3]],
        [part3, swapped(part3, "xl"), *updates[3]],
        dense_scratch,
    )
    arrived = row_copies(d2.reshape(4, 4, 16, 128), X4)
    pieces = exchange(value(2, arrived, 4), X4)
    y2, d1, d0 = call(
        functools.partial(push_wide_kernel, 2),
        [(16, widths[2]), (8, 8, 8, 128), (2, 64, 8, 128)],
        [place[2]],
        [pieces, d1, d0, *updates[2]],
        dense_scratch,
    )
    extra0 = swapped(jnp.where(lower, d0[1], d0[0]), "yl")
    arrived = row_copies(d1, ALL_X)
    pieces = exchange(value(1, arrived, 4), X4)
    y1, dense0 = call(
        push_top_kernel,
        [(8, widths[1]), (64, 8, 128)],
        [side1, place[1]],
        [pieces, d0, extra0, *updates[1]],
    )
    arrived = row_copies(dense0.reshape(8, 8, 8, 128), TOP)
    pieces = exchange(value(0, arrived, 8), TOP)

    def solved_share(level, minus, lead, n):
        rows, blocks = (8, 8) if level < 2 else (16, 4)
        out = call(
            functools.partial(solution_kernel, copies[level], minus),
            (8, blocks, rows, 128),
            [slots[level]],
            [*lead, *inverses[level]],
        )
        pieces = exchange(out, ("row",))
        if n == 0:
            return pieces
        return call(share_kernel, [(blocks, rows, 128), (n, blocks, rows, 128)], [], [pieces])

    x0, out = solved_share(0, 0, [pieces], 8)
    front0 = exchange(out, TOP).reshape(64, 8, 128)
    other0 = swapped(front0, "yl")
    pieces = exchange(
        call(pull_top_kernel, (4, 8, widths[1]), [place[1]], [front0, *updates[1]]), X4
    )
    x1, out = solved_share(1, 1, [y1, pieces], 8)
    front1 = exchange(out, ALL_X)
    pieces = exchange(
        call(
            functools.partial(pull_wide_kernel, 2),
            (4, 16, widths[2]),
            [side1, place[2]],
            [front0, other0, front1, *updates[2]],
            dense_scratch,
        ),
        X4,
    )
    x2, out = solved_share(2, 1, [y2, pieces], 4)
    front2 = exchange(out, X4).reshape(16, 16, 128)
    part3 = call(
        functools.partial(pull_wide_kernel, 3),
        (16, widths[3]),
        [side1, place[3]],
        [front0, other0, front1, front2, *updates[3]],
        dense_scratch,
    )
    pieces = solved_share(3, 2, [y3, part3, swapped(part3, "xl")], 0)

    kept3, given3 = call(last_kernel, [(2, 16, 128)] * 2, [slots_wide], [pieces])

    def merged(kept, given):
        return call(merge_kernel, (2, 32, 128), [core1], [kept, swapped(given, "core")])

    tops = jnp.stack([x0, x1])
    mine, given = jnp.where(lower, tops[:, :4], tops[:, 4:]), jnp.where(lower, tops[:, 4:], tops[:, :4])
    given = swapped(given, "yl")
    tops = jnp.where(
        lower, jnp.concatenate([mine, given], axis=2), jnp.concatenate([given, mine], axis=2)
    )
    solved = jnp.concatenate([tops, x2[None]])
    kept = jnp.where(first, solved[:, :2], solved[:, 2:])
    given = swapped(jnp.where(first, solved[:, 2:], solved[:, :2]), "core")
    outputs = jnp.where(
        first, jnp.concatenate([kept, given], axis=2), jnp.concatenate([given, kept], axis=2)
    )
    return outputs[0], outputs[1], outputs[2], merged(kept3, given3)


def solution(mesh):
    fine = Mesh(mesh.devices.reshape(2, 2, 2, 2, 2, 8), AXES)
    vector, matrix, index = P(LEAF, None, None), P(LEAF, None, "row"), P(LEAF)
    return jax.shard_map(
        body,
        mesh=fine,
        in_specs=(vector,) * 4 + (matrix,) * 7 + (index,) * 3,
        out_specs=(vector,) * 4,
        check_vma=False,
    )
```

```python
import functools
import math

import jax
import jax.numpy as jnp
from jax import lax
from jax.experimental import pallas as pl
from jax.experimental.pallas import tpu as pltpu
from jax.sharding import Mesh, PartitionSpec as P


AXES = ("yh", "yl", "xh", "xl", "core", "row")
LEAF = AXES[:5]
X4 = ("xh", "xl")
ALL_X = ("yl", "xh", "xl")
TOP = ("yh", "xh", "xl")
F32 = jnp.float32


def size_of(axes):
    total = 1
    for axis in axes:
        total *= lax.axis_size(axis)
    return total


def exchange(pieces, axes):
    return lax.all_to_all(pieces, axes, split_axis=0, concat_axis=0, tiled=True)


def swapped(x, axis):
    return lax.ppermute(x, axis, [(0, 1), (1, 0)])


def halves(x):
    high = x.astype(jnp.bfloat16)
    return high, (x - high.astype(F32)).astype(jnp.bfloat16)


def doubled(a):
    high = a.astype(jnp.bfloat16).astype(F32)
    return jnp.concatenate([high, a - high], axis=0).astype(jnp.bfloat16)


def product(rows, matrix, transposed):
    r = rows.shape[0]
    pair = doubled(rows)
    high, low = halves(matrix)
    dims = (((1,), (1 if transposed else 0,)), ((), ()))
    both = lax.dot_general(pair, high, dims, preferred_element_type=F32)
    both = both + lax.dot_general(pair, low, dims, preferred_element_type=F32)
    return both[:r] + both[r:]


def summed(ref, *index):
    total = ref[(0, *index)]
    for i in range(1, ref.shape[0]):
        total = total + ref[(i, *index)]
    return total


def call(kernel, outs, scalars, arrays, scratch=(), flops=2_000_000):
    size = sum(a.size for a in arrays) * 4
    single = isinstance(outs, tuple)
    shapes = [outs] if single else list(outs)
    size += sum(math.prod(s) for s in shapes) * 4
    room = size + sum(math.prod(s.shape) for s in scratch) * 4
    result = pl.pallas_call(
        kernel,
        out_shape=[jax.ShapeDtypeStruct(s, F32) for s in shapes],
        in_specs=[pl.BlockSpec(memory_space=pltpu.SMEM)] * len(scalars)
        + [pl.BlockSpec(memory_space=pltpu.VMEM)] * len(arrays),
        out_specs=[pl.BlockSpec(memory_space=pltpu.VMEM)] * len(shapes),
        scratch_shapes=list(scratch),
        compiler_params=pltpu.CompilerParams(vmem_limit_bytes=room + 3 * 2**20),
        cost_estimate=pl.CostEstimate(
            flops=flops, bytes_accessed=size, transcendentals=0
        ),
    )(*scalars, *arrays)
    return result[0] if single else result


def place_of(link):
    level, g = link >> 6, link & 63
    root = (g & 32) | (((g >> 2) & 3) << 3) | (((g >> 4) & 1) << 2) | (g & 3)
    return jnp.where(
        level == 0,
        48 + root,
        jnp.where(level == 1, 16 + (root & 31), link & 15),
    )


def places_of(refs, start, count):
    return lambda j: place_of(refs[j // count][start + j % count])


def blocks_slot(me, copies, k):
    core = me[0] ^ (k & 1)
    return core if copies == 2 else (me[1] ^ (k >> 1)) * 2 + core


def value_kernel(copies, start, arrives, me, *refs):
    refs = list(refs)
    arrived = refs.pop(0) if arrives else None
    sources, inverses, out = refs[:copies], refs[copies : 2 * copies], refs[2 * copies]
    count = 16 if copies == 2 else 8
    row = me[0] * 16 if copies == 2 else me[0] * 16 + me[1] * 8
    row = pl.multiple_of(row, count)
    total = None
    for k in range(copies):
        rows = []
        for b in range(2):
            w = sources[k][start + b, pl.ds(row, count)]
            if arrives:
                w = w - summed(arrived, blocks_slot(me, copies, k) * 2 + b)
            rows.append(w)
        width = inverses[k].shape[2]
        part = product(
            jnp.concatenate(rows, axis=1), inverses[k][...].reshape(256, width), False
        )
        total = part if total is None else total + part
    for i in range(out.shape[0]):
        out[i] = total


def contributions(solved, updates, add):
    j = 0
    for update in updates:
        for start in range(0, update.shape[0], 2):
            both = product(
                solved, update[start : start + 2].reshape(256, update.shape[2]), True
            )
            add(j, both[:, :128])
            add(j + 1, both[:, 128:])
            j += 2


def push_wide_kernel(level, own, core, *refs):
    places = places_of([own, core], 12 if level == 3 else 4, 8)
    if level == 3:
        pieces, refs = refs[:2], refs[2:]
        solved = pieces[0][...] + pieces[1][...]
        updates, (solved_ref, out2, out1, out0, dense) = refs[:2], refs[2:]
    else:
        pieces, old1, old0, refs = refs[0], refs[1], refs[2], refs[3:]
        solved = summed(pieces)
        updates, (solved_ref, out1, out0, dense) = refs[:2], refs[2:]
    solved_ref[...] = solved
    if level == 3:
        dense[...] = jnp.zeros(dense.shape, F32)
    else:
        dense[:, 16:48] = old1[...].reshape(2, 32, 8, 128)
        dense[:, 48:112] = old0[...]

    def add(j, block):
        place = places(j)
        dense[0, place] += block[:8]
        dense[1, place] += block[8:]

    contributions(solved, updates, add)
    if level == 3:
        out2[:, :8] = dense[0, 0:16]
        out2[:, 8:] = dense[1, 0:16]
    out1[...] = dense[:, 16:48].reshape(out1.shape)
    out0[...] = dense[:, 48:112]


def push_top_kernel(me, own, core, far, both, *refs):
    places = places_of([own, core, far, both], 0, 4)
    pieces, old0, extra0, refs = refs[0], refs[1], refs[2], refs[3:]
    updates, (solved_ref, dense) = refs[:4], refs[4:]
    solved = summed(pieces)
    solved_ref[...] = solved
    dense[...] = old0[me[1]] + extra0[...]

    def add(j, block):
        dense[places(j) - 48] += block

    contributions(solved, updates, add)


def copies_kernel(pieces, out):
    total = summed(pieces)
    for i in range(out.shape[0]):
        out[i] = total


def share_kernel(pieces, *refs):
    solved, out = refs[-2:]
    total = summed(pieces)
    if len(refs) == 3:
        solved[0] = refs[0][...]
        solved[1] = total
    else:
        solved[...] = total
    for i in range(out.shape[0]):
        out[i] = total


def solution_kernel(copies, minus, me, *refs):
    if minus == 0:
        refs, z = refs[1:], summed(refs[0])
    elif minus == 1:
        refs, z = refs[2:], refs[0][...] - summed(refs[1])
    else:
        refs, z = refs[3:], refs[0][...] - (refs[1][...] + refs[2][...])
    inverses, out = refs[:copies], refs[copies]
    for k in range(copies):
        both = product(z, inverses[k][...].reshape(256, inverses[k].shape[2]), True)
        slot = blocks_slot(me, copies, k) * 2
        for i in range(out.shape[0]):
            out[i, slot] = both[:, :128]
            out[i, slot + 1] = both[:, 128:]


def products_of(pick, updates):
    total, j = None, 0
    for update in updates:
        for start in range(0, update.shape[0], 2):
            rows = jnp.concatenate([pick(j), pick(j + 1)], axis=1)
            part = product(
                rows, update[start : start + 2].reshape(256, update.shape[2]), False
            )
            total = part if total is None else total + part
            j += 2
    return total


def pull_top_kernel(own, core, far, both, front, *refs):
    places = places_of([own, core, far, both], 0, 4)
    updates, out = refs[:4], refs[4]
    total = products_of(lambda j: front[places(j) - 48], updates)
    for i in range(out.shape[0]):
        out[i] = total


def pull_wide_kernel(level, me, own, core, own0, other0, front1, *refs):
    places = places_of([own, core], 12 if level == 3 else 4, 8)
    if level == 3:
        front2, refs = refs[0], refs[1:]
    updates, (out, dense) = refs[:2], refs[2:]
    dense[me[1], 48:112] = own0[...]
    dense[1 - me[1], 48:112] = other0[...]
    dense[:, 16:48] = front1[...].reshape(2, 32, 8, 128)
    if level == 3:
        dense[0, 0:16] = front2[:, :8]
        dense[1, 0:16] = front2[:, 8:]
    total = products_of(
        lambda j: jnp.concatenate([dense[0, places(j)], dense[1, places(j)]], axis=0),
        updates,
    )
    if level == 3:
        out[...] = total
    else:
        for i in range(out.shape[0]):
            out[i] = total


def sum_kernel(pieces, out):
    out[...] = summed(pieces)


def merge_kernel(me, mine, theirs, out):
    for b in range(2):
        block = me[0] * 2 + b
        out[b, pl.ds(pl.multiple_of(me[0] * 16, 16), 16)] = mine[block]
        out[b, pl.ds(pl.multiple_of((1 - me[0]) * 16, 16), 16)] = theirs[block]


def merge_top_kernel(me, *refs):
    tops, outs = refs[:4], refs[4:]
    for k in range(4):
        row = (me[0] ^ (k & 1)) * 16 + (me[1] ^ (k >> 1)) * 8
        for level in range(2):
            for b in range(2):
                block = (me[1] * 2 + me[0]) * 2 + b
                outs[level][b, pl.ds(pl.multiple_of(row, 8), 8)] = tops[k][level, block]


def body(*args):
    sources, inverse = args[0:4], args[4:8]
    update, links = [None, *args[8:11]], args[11:14]
    core, side = lax.axis_index("core"), lax.axis_index("yl")
    lower = side == 0
    me = jnp.stack([core, side]).astype(jnp.int32)

    def pair(x):
        return [x, swapped(x, "core")]

    def quad(x):
        return [*pair(x), *pair(swapped(x, "yl"))]

    source_of, inverses, updates = [None] * 4, [None] * 4, [None] * 4
    source_of[3], inverses[3] = pair(sources[3]), pair(inverse[3])
    updates[3] = pair(update[3])
    index = quad(jnp.concatenate(links))
    source_of[2], inverses[2] = pair(sources[2]), pair(inverse[2])
    updates[2] = pair(update[2])
    inverses[1], updates[1] = quad(inverse[1]), quad(update[1])
    inverses[0] = quad(inverse[0])
    source_of[0] = source_of[1] = quad(jnp.concatenate(sources[:2]))
    copies = [4, 4, 2, 2]
    widths = [i.shape[2] for i in inverse]

    def value(level, arrived, n):
        rows = 8 if level < 2 else 16
        lead = [] if arrived is None else [arrived]
        return call(
            functools.partial(
                value_kernel, copies[level], 2 * (level == 1), arrived is not None
            ),
            (n, rows, widths[level]),
            [me],
            [*lead, *source_of[level], *inverses[level]],
        )

    def row_copies(pieces, axes):
        pieces = exchange(pieces, axes)
        n = pieces.shape[0]
        out = call(copies_kernel, (8, *pieces.shape[1:]), [], [pieces])
        return exchange(out, ("row",))

    dense_scratch = [pltpu.VMEM((2, 112, 8, 128), F32)]
    part3 = value(3, None, 1)[0]
    y3, d2, d1, d0 = call(
        functools.partial(push_wide_kernel, 3),
        [(16, widths[3]), (16, 16, 128), (8, 8, 8, 128), (2, 64, 8, 128)],
        index[:2],
        [part3, swapped(part3, "xl"), *updates[3]],
        dense_scratch,
    )
    arrived = row_copies(d2.reshape(4, 4, 16, 128), X4)
    pieces = exchange(value(2, arrived, 4), X4)
    y2, d1, d0 = call(
        functools.partial(push_wide_kernel, 2),
        [(16, widths[2]), (8, 8, 8, 128), (2, 64, 8, 128)],
        index[:2],
        [pieces, d1, d0, *updates[2]],
        dense_scratch,
    )
    extra0 = swapped(jnp.where(lower, d0[1], d0[0]), "yl")
    arrived = row_copies(d1, ALL_X)
    pieces = exchange(value(1, arrived, 4), X4)
    y1, dense0 = call(
        push_top_kernel,
        [(8, widths[1]), (64, 8, 128)],
        [me, *index],
        [pieces, d0, extra0, *updates[1]],
    )
    arrived = row_copies(dense0.reshape(8, 8, 8, 128), TOP)
    pieces = exchange(value(0, arrived, 8), TOP)

    def solved_share(level, minus, lead, n, before=()):
        rows, blocks = (8, 8) if level < 2 else (16, 4)
        out = call(
            functools.partial(solution_kernel, copies[level], minus),
            (8, blocks, rows, 128),
            [me],
            [*lead, *inverses[level]],
        )
        pieces = exchange(out, ("row",))
        if n == 0:
            return pieces
        kept = (2,) * len(before) + (blocks, rows, 128)
        return call(share_kernel, [kept, (n, blocks, rows, 128)], [], [pieces, *before])

    x0, out = solved_share(0, 0, [pieces], 8)
    front0 = exchange(out, TOP).reshape(64, 8, 128)
    other0 = swapped(front0, "yl")
    pieces = exchange(
        call(pull_top_kernel, (4, 8, widths[1]), index, [front0, *updates[1]]), X4
    )
    tops, out = solved_share(1, 1, [y1, pieces], 8, [x0])
    top0, top1 = call(merge_top_kernel, [(2, 32, 128)] * 2, [me], quad(tops))
    front1 = exchange(out, ALL_X)
    pieces = exchange(
        call(
            functools.partial(pull_wide_kernel, 2),
            (4, 16, widths[2]),
            [me, *index[:2]],
            [front0, other0, front1, *updates[2]],
            dense_scratch,
        ),
        X4,
    )
    x2, out = solved_share(2, 1, [y2, pieces], 4)
    front2 = exchange(out, X4).reshape(16, 16, 128)
    part3 = call(
        functools.partial(pull_wide_kernel, 3),
        (16, widths[3]),
        [me, *index[:2]],
        [front0, other0, front1, front2, *updates[3]],
        dense_scratch,
    )
    pieces = solved_share(3, 2, [y3, part3, swapped(part3, "xl")], 0)

    x3 = call(sum_kernel, (4, 16, 128), [], [pieces])
    deep = [call(merge_kernel, (2, 32, 128), [me], pair(x)) for x in (x2, x3)]
    return top0, top1, *deep


def solution(mesh):
    fine = Mesh(mesh.devices.reshape(2, 2, 2, 2, 2, 8), AXES)
    vector, matrix, index = P(LEAF, None, None), P(LEAF, None, "row"), P(LEAF)
    return jax.shard_map(
        body,
        mesh=fine,
        in_specs=(vector,) * 4 + (matrix,) * 7 + (index,) * 3,
        out_specs=(vector,) * 4,
        check_vma=False,
    )
```

```python
import functools
import math

import jax
import jax.numpy as jnp
from jax import lax
from jax.experimental import pallas as pl
from jax.experimental.pallas import tpu as pltpu
from jax.sharding import Mesh, PartitionSpec as P


AXES = ("yh", "yl", "xh", "xl", "core", "row")
LEAF = AXES[:5]
X4 = ("xh", "xl")
Y4 = ("yh", "yl")
CHIPS = [Y4 + X4, ("yl",) + X4, X4]
F32 = jnp.float32


def size_of(axes):
    total = 1
    for axis in axes:
        total *= lax.axis_size(axis)
    return total


def exchange(pieces, axes):
    return lax.all_to_all(pieces, axes, split_axis=0, concat_axis=0, tiled=True)


def swapped(x, axis):
    return lax.ppermute(x, axis, [(0, 1), (1, 0)])


def halves(x):
    high = x.astype(jnp.bfloat16)
    return high, (x - high.astype(F32)).astype(jnp.bfloat16)


def doubled(a):
    high = a.astype(jnp.bfloat16).astype(F32)
    return jnp.concatenate([high, a - high], axis=0).astype(jnp.bfloat16)


def product(rows, matrix, transposed):
    r = rows.shape[0]
    pair = doubled(rows)
    high, low = halves(matrix)
    dims = (((1,), (1 if transposed else 0,)), ((), ()))
    both = lax.dot_general(pair, high, dims, preferred_element_type=F32)
    both = both + lax.dot_general(pair, low, dims, preferred_element_type=F32)
    return both[:r] + both[r:]


def summed(ref, *index):
    total = ref[(0, *index)]
    for i in range(1, ref.shape[0]):
        total = total + ref[(i, *index)]
    return total


def call(kernel, outs, scalars, arrays, scratch=(), flops=2_000_000):
    size = sum(a.size for a in arrays) * 4
    single = isinstance(outs, tuple)
    shapes = [outs] if single else list(outs)
    size += sum(math.prod(s) for s in shapes) * 4
    room = size + sum(math.prod(s.shape) for s in scratch) * 4
    result = pl.pallas_call(
        kernel,
        out_shape=[jax.ShapeDtypeStruct(s, F32) for s in shapes],
        in_specs=[pl.BlockSpec(memory_space=pltpu.SMEM)] * len(scalars)
        + [pl.BlockSpec(memory_space=pltpu.VMEM)] * len(arrays),
        out_specs=[pl.BlockSpec(memory_space=pltpu.VMEM)] * len(shapes),
        scratch_shapes=list(scratch),
        compiler_params=pltpu.CompilerParams(vmem_limit_bytes=room + 3 * 2**20),
        cost_estimate=pl.CostEstimate(
            flops=flops, bytes_accessed=size, transcendentals=0
        ),
    )(*scalars, *arrays)
    return result[0] if single else result


def place_of(link):
    level = link >> 6
    return jnp.where(
        level == 0,
        48 + link,
        jnp.where(level == 1, 16 + (link & 31), link & 15),
    )


def places_of(refs):
    count = refs[0].shape[0]
    return lambda j: place_of(refs[j // count][j % count])


def value_kernel(arrives, me, *refs):
    refs = list(refs)
    arrived = refs.pop(0) if arrives else None
    sources, inverses, out = refs[:2], refs[2:4], refs[4]
    row = pl.multiple_of(me[0] * 16, 16)
    total = None
    for k in range(2):
        rows = []
        for b in range(2):
            w = sources[k][b, pl.ds(row, 16)]
            if arrives:
                w = w - summed(arrived, (me[0] ^ k) * 2 + b)
            rows.append(w)
        width = inverses[k].shape[2]
        part = product(
            jnp.concatenate(rows, axis=1), inverses[k][...].reshape(256, width), False
        )
        total = part if total is None else total + part
    for i in range(out.shape[0]):
        out[i] = total


def push_kernel(level, own, other, *refs):
    places = places_of([own, other])
    if level == 3:
        solved, refs = refs[0][...] + refs[1][...], refs[2:]
    else:
        solved, old, refs = summed(refs[0]), refs[1], refs[2:]
    updates, refs = refs[:2], refs[2:]
    solved_ref, dense = refs[0], refs[-1]
    solved_ref[...] = solved
    if level == 3:
        dense[...] = jnp.zeros(dense.shape, F32)
    elif level == 2:
        dense[16:112] = old[...]
    else:
        dense[48:112] = old[...]
    j = 0
    for update in updates:
        for start in range(0, update.shape[0], 2):
            both = product(
                solved, update[start : start + 2].reshape(256, update.shape[2]), True
            )
            dense[places(j)] += both[:, :128]
            dense[places(j + 1)] += both[:, 128:]
            j += 2
    if level == 3:
        refs[1][...] = dense[0:16]
        refs[2][...] = dense[16:112]
    elif level == 2:
        refs[1][...] = dense[16:48]
        refs[2][...] = dense[48:112]
    else:
        refs[1][...] = dense[48:112]


def copies_kernel(pieces, out):
    total = summed(pieces)
    for i in range(out.shape[0]):
        out[i] = total


def share_kernel(pieces, solved, out):
    total = summed(pieces)
    solved[...] = total
    for i in range(out.shape[0]):
        out[i] = total


def solution_kernel(minus, me, *refs):
    if minus == 0:
        refs, z = refs[1:], summed(refs[0])
    elif minus == 1:
        refs, z = refs[2:], refs[0][...] - summed(refs[1])
    else:
        refs, z = refs[3:], refs[0][...] - (refs[1][...] + refs[2][...])
    inverses, out = refs[:2], refs[2]
    for k in range(2):
        both = product(z, inverses[k][...].reshape(256, inverses[k].shape[2]), True)
        slot = (me[0] ^ k) * 2
        for i in range(out.shape[0]):
            out[i, slot] = both[:, :128]
            out[i, slot + 1] = both[:, 128:]


def pull_kernel(level, own, other, *refs):
    places = places_of([own, other])
    fronts, updates, refs = refs[:level], refs[level : level + 2], refs[level + 2 :]
    out = refs[0]
    if level == 1:
        front, base = fronts[0], 48
    else:
        front, base = refs[1], 0
        front[48:112] = fronts[0][...]
        front[16:48] = fronts[1][...]
        if level == 3:
            front[0:16] = fronts[2][...]
    total, j = None, 0
    for update in updates:
        for start in range(0, update.shape[0], 2):
            rows = jnp.concatenate(
                [front[places(j) - base], front[places(j + 1) - base]], axis=1
            )
            part = product(
                rows, update[start : start + 2].reshape(256, update.shape[2]), False
            )
            total = part if total is None else total + part
            j += 2
    for i in range(out.shape[0]):
        out[i] = total


def last_kernel(me, *refs):
    solved, pieces, kept, given = refs[:3], refs[3], refs[4], refs[5]
    for out, core in ((kept, me[0]), (given, 1 - me[0])):
        for b in range(2):
            block = core * 2 + b
            for level in range(3):
                out[level, b] = solved[level][block]
            out[3, b] = summed(pieces, block)


def merge_kernel(me, kept, given, *outs):
    mine = pl.ds(pl.multiple_of(me[0] * 16, 16), 16)
    theirs = pl.ds(pl.multiple_of((1 - me[0]) * 16, 16), 16)
    for level in range(4):
        outs[level][:, mine] = kept[level]
        outs[level][:, theirs] = given[level]


def body(*args):
    sources, inverse = args[0:4], args[4:8]
    update, links = [None, *args[8:11]], [None, *args[11:14]]
    me = lax.axis_index("core").astype(jnp.int32).reshape(1)
    widths = [i.shape[2] for i in inverse]
    rows = 16

    def pair(x):
        return [x, swapped(x, "core")]

    source_of, inverses, updates, index = ([None] * 4 for _ in range(4))
    for level in (3, 2, 1, 0):
        source_of[level] = pair(sources[level])
        inverses[level] = pair(inverse[level])
        if level:
            index[level] = pair(links[level])
            updates[level] = pair(update[level])

    def value(level, lead, n):
        return call(
            functools.partial(value_kernel, bool(lead)),
            (n, rows, widths[level]),
            [me],
            [*lead, *source_of[level], *inverses[level]],
        )

    def push(level, lead, sizes, scratch):
        return call(
            functools.partial(push_kernel, level),
            [(rows, widths[level]), *((n, rows, 128) for n in sizes)],
            index[level],
            [*lead, *updates[level]],
            [pltpu.VMEM((112, rows, 128), F32)] if scratch else [],
        )

    def copied(pieces, n):
        return call(copies_kernel, (n, *pieces.shape[1:]), [], [pieces])

    def delivered(dense, level):
        pieces = exchange(dense.reshape(-1, 4, rows, 128), CHIPS[level])
        return exchange(copied(pieces, 8), ("row",))

    part3 = value(3, [], 1)[0]
    y3, dense, rest = push(3, [part3, swapped(part3, "xl")], (16, 96), True)
    dense, source_of, inverses, updates, index = lax.optimization_barrier(
        (dense, source_of, inverses, updates, index)
    )
    pieces = exchange(value(2, [delivered(dense, 2)], 4), X4)
    y2, dense, rest = push(2, [pieces, rest], (32, 64), True)
    arrived = delivered(dense, 1)
    pieces = exchange(value(1, [arrived], 8), CHIPS[1])
    y1, dense = push(1, [pieces, rest], (64,), True)
    arrived = delivered(dense, 0)
    pieces = exchange(value(0, [arrived], 4), X4)
    pieces = exchange(copied(pieces, 4), Y4)

    def row_pieces(level, minus, lead):
        out = call(
            functools.partial(solution_kernel, minus),
            (8, 4, rows, 128),
            [me],
            [*lead, *inverses[level]],
        )
        return exchange(out, ("row",))

    def shared(pieces, level):
        n = size_of(CHIPS[level])
        solved, out = call(
            share_kernel, [(4, rows, 128), (n, 4, rows, 128)], [], [pieces]
        )
        return solved, exchange(out, CHIPS[level]).reshape(-1, rows, 128)

    def pull(level, fronts, n):
        return call(
            functools.partial(pull_kernel, level),
            (n, rows, widths[level]),
            index[level],
            [*fronts, *updates[level]],
            [pltpu.VMEM((112, rows, 128), F32)] if level > 1 else [],
        )

    x0, front0 = shared(row_pieces(0, 0, [pieces]), 0)
    pieces = exchange(pull(1, [front0], 8), CHIPS[1])
    x1, front1 = shared(row_pieces(1, 1, [y1, pieces]), 1)
    pieces = exchange(pull(2, [front0, front1], 4), X4)
    x2, front2 = shared(row_pieces(2, 1, [y2, pieces]), 2)
    part3 = pull(3, [front0, front1, front2], 1)[0]
    pieces = row_pieces(3, 2, [y3, part3, swapped(part3, "xl")])
    kept, given = call(
        last_kernel, [(4, 2, rows, 128)] * 2, [me], [x0, x1, x2, pieces]
    )
    return tuple(
        call(merge_kernel, [(2, 32, 128)] * 4, [me], [kept, swapped(given, "core")])
    )


def solution(mesh):
    fine = Mesh(mesh.devices.reshape(2, 2, 2, 2, 2, 8), AXES)
    vector, matrix, index = P(LEAF, None, None), P(LEAF, None, "row"), P(LEAF)
    return jax.shard_map(
        body,
        mesh=fine,
        in_specs=(vector,) * 4 + (matrix,) * 7 + (index,) * 3,
        out_specs=(vector,) * 4,
        check_vma=False,
    )
```

```python
import functools
import math

import jax
import jax.numpy as jnp
from jax import lax
from jax.experimental import pallas as pl
from jax.experimental.pallas import tpu as pltpu
from jax.sharding import Mesh, PartitionSpec as P


AXES = ("yh", "yl", "xh", "xl", "core", "row")
LEAF = AXES[:5]
X4 = ("xh", "xl")
Y4 = ("yh", "yl")
CHIPS = [Y4 + X4, ("yl",) + X4, X4]
F32 = jnp.float32


def size_of(axes):
    total = 1
    for axis in axes:
        total *= lax.axis_size(axis)
    return total


def exchange(pieces, axes):
    return lax.all_to_all(pieces, axes, split_axis=0, concat_axis=0, tiled=True)


def swapped(x, axis):
    return lax.ppermute(x, axis, [(0, 1), (1, 0)])


def halves(x):
    high = x.astype(jnp.bfloat16)
    return high, (x - high.astype(F32)).astype(jnp.bfloat16)


def doubled(a):
    high = a.astype(jnp.bfloat16).astype(F32)
    return jnp.concatenate([high, a - high], axis=0).astype(jnp.bfloat16)


def product(rows, matrix, transposed):
    r = rows.shape[0]
    pair = doubled(rows)
    high, low = halves(matrix)
    dims = (((1,), (1 if transposed else 0,)), ((), ()))
    both = lax.dot_general(pair, high, dims, preferred_element_type=F32)
    both = both + lax.dot_general(pair, low, dims, preferred_element_type=F32)
    return both[:r] + both[r:]


def summed(ref, *index):
    total = ref[(0, *index)]
    for i in range(1, ref.shape[0]):
        total = total + ref[(i, *index)]
    return total


def call(kernel, outs, scalars, arrays, scratch=(), flops=2_000_000):
    size = sum(a.size for a in arrays) * 4
    single = isinstance(outs, tuple)
    shapes = [outs] if single else list(outs)
    size += sum(math.prod(s) for s in shapes) * 4
    room = size + sum(math.prod(s.shape) for s in scratch) * 4
    result = pl.pallas_call(
        kernel,
        out_shape=[jax.ShapeDtypeStruct(s, F32) for s in shapes],
        in_specs=[pl.BlockSpec(memory_space=pltpu.SMEM)] * len(scalars)
        + [pl.BlockSpec(memory_space=pltpu.VMEM)] * len(arrays),
        out_specs=[pl.BlockSpec(memory_space=pltpu.VMEM)] * len(shapes),
        scratch_shapes=list(scratch),
        compiler_params=pltpu.CompilerParams(vmem_limit_bytes=room + 3 * 2**20),
        cost_estimate=pl.CostEstimate(
            flops=flops, bytes_accessed=size, transcendentals=0
        ),
    )(*scalars, *arrays)
    return result[0] if single else result


def place_of(link):
    level = link >> 6
    return jnp.where(
        level == 0,
        48 + link,
        jnp.where(level == 1, 16 + (link & 31), link & 15),
    )


def places_of(refs):
    count = refs[0].shape[0]
    return lambda j: place_of(refs[j // count][j % count])


def value_kernel(arrives, me, *refs):
    refs = list(refs)
    arrived = refs.pop(0) if arrives else None
    sources, inverses, out = refs[:2], refs[2:4], refs[4]
    row = pl.multiple_of(me[0] * 16, 16)
    total = None
    for k in range(2):
        rows = []
        for b in range(2):
            w = sources[k][b, pl.ds(row, 16)]
            if arrives:
                w = w - summed(arrived, (me[0] ^ k) * 2 + b)
            rows.append(w)
        width = inverses[k].shape[2]
        part = product(
            jnp.concatenate(rows, axis=1), inverses[k][...].reshape(256, width), False
        )
        total = part if total is None else total + part
    for i in range(out.shape[0]):
        out[i] = total


def push_kernel(level, own, other, *refs):
    places = places_of([own, other])
    if level == 3:
        solved, refs = refs[0][...] + refs[1][...], refs[2:]
    else:
        solved, old, refs = summed(refs[0]), refs[1], refs[2:]
    updates, refs = refs[:2], refs[2:]
    solved_ref, dense = refs[0], refs[-1]
    solved_ref[...] = solved
    if level == 3:
        dense[...] = jnp.zeros(dense.shape, F32)
    elif level == 2:
        dense[16:112] = old[...]
    else:
        dense[48:112] = old[...]
    j = 0
    for update in updates:
        for start in range(0, update.shape[0], 2):
            both = product(
                solved, update[start : start + 2].reshape(256, update.shape[2]), True
            )
            dense[places(j)] += both[:, :128]
            dense[places(j + 1)] += both[:, 128:]
            j += 2
    if level == 3:
        refs[1][...] = dense[0:16]
        refs[2][...] = dense[16:112]
    elif level == 2:
        refs[1][...] = dense[16:48]
        refs[2][...] = dense[48:112]
    else:
        refs[1][...] = dense[48:112]


def copies_kernel(pieces, out):
    total = summed(pieces)
    for i in range(out.shape[0]):
        out[i] = total


def share_kernel(pieces, solved, out):
    total = summed(pieces)
    solved[...] = total
    for i in range(out.shape[0]):
        out[i] = total


def solution_kernel(minus, me, *refs):
    if minus == 0:
        refs, z = refs[1:], summed(refs[0])
    elif minus == 1:
        refs, z = refs[2:], refs[0][...] - summed(refs[1])
    else:
        refs, z = refs[3:], refs[0][...] - (refs[1][...] + refs[2][...])
    inverses, out = refs[:2], refs[2]
    for k in range(2):
        both = product(z, inverses[k][...].reshape(256, inverses[k].shape[2]), True)
        slot = (me[0] ^ k) * 2
        for i in range(out.shape[0]):
            out[i, slot] = both[:, :128]
            out[i, slot + 1] = both[:, 128:]


def pull_kernel(level, own, other, *refs):
    places = places_of([own, other])
    fronts, updates, refs = refs[:level], refs[level : level + 2], refs[level + 2 :]
    out = refs[0]
    if level == 1:
        front, base = fronts[0], 48
    else:
        front, base = refs[1], 0
        front[48:112] = fronts[0][...]
        front[16:48] = fronts[1][...]
        if level == 3:
            front[0:16] = fronts[2][...]
    total, j = None, 0
    for update in updates:
        for start in range(0, update.shape[0], 2):
            rows = jnp.concatenate(
                [front[places(j) - base], front[places(j + 1) - base]], axis=1
            )
            part = product(
                rows, update[start : start + 2].reshape(256, update.shape[2]), False
            )
            total = part if total is None else total + part
            j += 2
    for i in range(out.shape[0]):
        out[i] = total


def last_kernel(me, *refs):
    solved, pieces, kept, given = refs[:3], refs[3], refs[4], refs[5]
    for out, core in ((kept, me[0]), (given, 1 - me[0])):
        for b in range(2):
            block = core * 2 + b
            for level in range(3):
                out[level, b] = solved[level][block]
            out[3, b] = summed(pieces, block)


def merge_kernel(me, kept, given, *outs):
    mine = pl.ds(pl.multiple_of(me[0] * 16, 16), 16)
    theirs = pl.ds(pl.multiple_of((1 - me[0]) * 16, 16), 16)
    for level in range(4):
        outs[level][:, mine] = kept[level]
        outs[level][:, theirs] = given[level]


def body(*args):
    sources, inverse = args[0:4], args[4:8]
    update, links = [None, *args[8:11]], [None, *args[11:14]]
    me = lax.axis_index("core").astype(jnp.int32).reshape(1)
    widths = [i.shape[2] for i in inverse]
    rows = 16

    def pair(x):
        return [x, swapped(x, "core")]

    source_of, inverses, updates, index = ([None] * 4 for _ in range(4))
    source_of[3], inverses[3] = pair(sources[3]), pair(inverse[3])
    updates[3], index[3] = pair(update[3]), pair(links[3])
    rest = (sources[:3], inverse[:3], update[1:3], links[1:3])
    early = (source_of[3][1], inverses[3][1], updates[3][1])
    rest = lax.optimization_barrier((rest, early))[0]
    for level in (2, 1, 0):
        source_of[level], inverses[level] = pair(rest[0][level]), pair(rest[1][level])
        if level:
            updates[level], index[level] = pair(rest[2][level - 1]), pair(rest[3][level - 1])

    def value(level, lead, n):
        return call(
            functools.partial(value_kernel, bool(lead)),
            (n, rows, widths[level]),
            [me],
            [*lead, *source_of[level], *inverses[level]],
        )

    def push(level, lead, sizes, scratch):
        return call(
            functools.partial(push_kernel, level),
            [(rows, widths[level]), *((n, rows, 128) for n in sizes)],
            index[level],
            [*lead, *updates[level]],
            [pltpu.VMEM((112, rows, 128), F32)] if scratch else [],
        )

    def copied(pieces, n):
        return call(copies_kernel, (n, *pieces.shape[1:]), [], [pieces])

    def delivered(dense, level):
        pieces = exchange(dense.reshape(-1, 4, rows, 128), CHIPS[level])
        return exchange(copied(pieces, 8), ("row",))

    part3 = value(3, [], 1)[0]
    y3, dense, rest = push(3, [part3, swapped(part3, "xl")], (16, 96), True)
    dense, source_of, inverses, updates, index = lax.optimization_barrier(
        (dense, source_of, inverses, updates, index)
    )
    pieces = exchange(value(2, [delivered(dense, 2)], 4), X4)
    y2, dense, rest = push(2, [pieces, rest], (32, 64), True)
    arrived = delivered(dense, 1)
    pieces = exchange(value(1, [arrived], 8), CHIPS[1])
    y1, dense = push(1, [pieces, rest], (64,), True)
    arrived = delivered(dense, 0)
    pieces = exchange(value(0, [arrived], 4), X4)
    pieces = exchange(copied(pieces, 4), Y4)

    def row_pieces(level, minus, lead):
        out = call(
            functools.partial(solution_kernel, minus),
            (8, 4, rows, 128),
            [me],
            [*lead, *inverses[level]],
        )
        return exchange(out, ("row",))

    def shared(pieces, level):
        n = size_of(CHIPS[level])
        solved, out = call(
            share_kernel, [(4, rows, 128), (n, 4, rows, 128)], [], [pieces]
        )
        return solved, exchange(out, CHIPS[level]).reshape(-1, rows, 128)

    def pull(level, fronts, n):
        return call(
            functools.partial(pull_kernel, level),
            (n, rows, widths[level]),
            index[level],
            [*fronts, *updates[level]],
            [pltpu.VMEM((112, rows, 128), F32)] if level > 1 else [],
        )

    x0, front0 = shared(row_pieces(0, 0, [pieces]), 0)
    pieces = exchange(pull(1, [front0], 8), CHIPS[1])
    x1, front1 = shared(row_pieces(1, 1, [y1, pieces]), 1)
    pieces = exchange(pull(2, [front0, front1], 4), X4)
    x2, front2 = shared(row_pieces(2, 1, [y2, pieces]), 2)
    part3 = pull(3, [front0, front1, front2], 1)[0]
    pieces = row_pieces(3, 2, [y3, part3, swapped(part3, "xl")])
    kept, given = call(
        last_kernel, [(4, 2, rows, 128)] * 2, [me], [x0, x1, x2, pieces]
    )
    return tuple(
        call(merge_kernel, [(2, 32, 128)] * 4, [me], [kept, swapped(given, "core")])
    )


def solution(mesh):
    fine = Mesh(mesh.devices.reshape(2, 2, 2, 2, 2, 8), AXES)
    vector, matrix, index = P(LEAF, None, None), P(LEAF, None, "row"), P(LEAF)
    return jax.shard_map(
        body,
        mesh=fine,
        in_specs=(vector,) * 4 + (matrix,) * 7 + (index,) * 3,
        out_specs=(vector,) * 4,
        check_vma=False,
    )
```

```python
import functools
import math

import jax
import jax.numpy as jnp
from jax import lax
from jax.experimental import pallas as pl
from jax.experimental.pallas import tpu as pltpu
from jax.sharding import Mesh, PartitionSpec as P


AXES = ("yh", "yl", "xh", "xl", "core", "row")
LEAF = AXES[:5]
X4 = ("xh", "xl")
Y4 = ("yh", "yl")
CHIPS = [Y4 + X4, ("yl",) + X4, X4]
F32 = jnp.float32


def size_of(axes):
    total = 1
    for axis in axes:
        total *= lax.axis_size(axis)
    return total


def exchange(pieces, axes):
    return lax.all_to_all(pieces, axes, split_axis=0, concat_axis=0, tiled=True)


def swapped(x, axis):
    return lax.ppermute(x, axis, [(0, 1), (1, 0)])


def halves(x):
    high = x.astype(jnp.bfloat16)
    return high, (x - high.astype(F32)).astype(jnp.bfloat16)


def doubled(a):
    high = a.astype(jnp.bfloat16).astype(F32)
    return jnp.concatenate([high, a - high], axis=0).astype(jnp.bfloat16)


def product(rows, matrix, transposed):
    r = rows.shape[0]
    pair = doubled(rows)
    high, low = halves(matrix)
    dims = (((1,), (1 if transposed else 0,)), ((), ()))
    both = lax.dot_general(pair, high, dims, preferred_element_type=F32)
    both = both + lax.dot_general(pair, low, dims, preferred_element_type=F32)
    return both[:r] + both[r:]


def summed(ref, *index):
    total = ref[(0, *index)]
    for i in range(1, ref.shape[0]):
        total = total + ref[(i, *index)]
    return total


def fetching(kernel, arrays, count, outs, *refs):
    head, far = refs[: arrays - count], refs[arrays - count : arrays]
    near, sems = refs[-count - 1 : -1], refs[-1]
    copies = [
        pltpu.make_async_copy(far[i], near[i], sems.at[i]) for i in range(count)
    ]
    for copy in copies:
        copy.start()
    for copy in copies:
        copy.wait()
    kernel(*head, *near, *refs[arrays : -count - 1])


def call(kernel, outs, scalars, arrays, scratch=(), flops=2_000_000, fetch=0):
    size = sum(a.size for a in arrays) * 4
    single = isinstance(outs, tuple)
    shapes = [outs] if single else list(outs)
    size += sum(math.prod(s) for s in shapes) * 4
    room = size + sum(math.prod(s.shape) for s in scratch) * 4
    spaces = [pltpu.VMEM] * (len(arrays) - fetch) + [pltpu.HBM] * fetch
    if fetch:
        kernel = functools.partial(
            fetching, kernel, len(scalars) + len(arrays), fetch, len(shapes)
        )
        scratch = [
            *scratch,
            *(pltpu.VMEM(a.shape, F32) for a in arrays[-fetch:]),
            pltpu.SemaphoreType.DMA((fetch,)),
        ]
    result = pl.pallas_call(
        kernel,
        out_shape=[jax.ShapeDtypeStruct(s, F32) for s in shapes],
        in_specs=[pl.BlockSpec(memory_space=pltpu.SMEM)] * len(scalars)
        + [pl.BlockSpec(memory_space=space) for space in spaces],
        out_specs=[pl.BlockSpec(memory_space=pltpu.VMEM)] * len(shapes),
        scratch_shapes=list(scratch),
        compiler_params=pltpu.CompilerParams(vmem_limit_bytes=62 * 2**20 if fetch else room + 3 * 2**20),
        cost_estimate=pl.CostEstimate(
            flops=flops, bytes_accessed=size, transcendentals=0
        ),
    )(*scalars, *arrays)
    return result[0] if single else result


def place_of(link):
    level = link >> 6
    return jnp.where(
        level == 0,
        48 + link,
        jnp.where(level == 1, 16 + (link & 31), link & 15),
    )


def places_of(refs):
    count = refs[0].shape[0]
    return lambda j: place_of(refs[j // count][j % count])


def value_kernel(arrives, me, *refs):
    refs = list(refs)
    arrived = refs.pop(0) if arrives else None
    sources, inverses, out = refs[:2], refs[2:4], refs[4]
    row = pl.multiple_of(me[0] * 16, 16)
    total = None
    for k in range(2):
        rows = []
        for b in range(2):
            w = sources[k][b, pl.ds(row, 16)]
            if arrives:
                w = w - summed(arrived, (me[0] ^ k) * 2 + b)
            rows.append(w)
        width = inverses[k].shape[2]
        part = product(
            jnp.concatenate(rows, axis=1), inverses[k][...].reshape(256, width), False
        )
        total = part if total is None else total + part
    for i in range(out.shape[0]):
        out[i] = total


def push_kernel(level, own, other, *refs):
    places = places_of([own, other])
    if level == 3:
        solved, refs = refs[0][...] + refs[1][...], refs[2:]
    else:
        solved, old, refs = summed(refs[0]), refs[1], refs[2:]
    updates, refs = refs[:2], refs[2:]
    solved_ref, dense = refs[0], refs[-1]
    solved_ref[...] = solved
    if level == 3:
        dense[...] = jnp.zeros(dense.shape, F32)
    elif level == 2:
        dense[16:112] = old[...]
    else:
        dense[48:112] = old[...]
    j = 0
    for update in updates:
        for start in range(0, update.shape[0], 2):
            both = product(
                solved, update[start : start + 2].reshape(256, update.shape[2]), True
            )
            dense[places(j)] += both[:, :128]
            dense[places(j + 1)] += both[:, 128:]
            j += 2
    if level == 3:
        refs[1][...] = dense[0:16]
        refs[2][...] = dense[16:112]
    elif level == 2:
        refs[1][...] = dense[16:48]
        refs[2][...] = dense[48:112]
    else:
        refs[1][...] = dense[48:112]


def copies_kernel(pieces, out):
    total = summed(pieces)
    for i in range(out.shape[0]):
        out[i] = total


def share_kernel(pieces, solved, out):
    total = summed(pieces)
    solved[...] = total
    for i in range(out.shape[0]):
        out[i] = total


def solution_kernel(minus, me, *refs):
    if minus == 0:
        refs, z = refs[1:], summed(refs[0])
    elif minus == 1:
        refs, z = refs[2:], refs[0][...] - summed(refs[1])
    else:
        refs, z = refs[3:], refs[0][...] - (refs[1][...] + refs[2][...])
    inverses, out = refs[:2], refs[2]
    for k in range(2):
        both = product(z, inverses[k][...].reshape(256, inverses[k].shape[2]), True)
        slot = (me[0] ^ k) * 2
        for i in range(out.shape[0]):
            out[i, slot] = both[:, :128]
            out[i, slot + 1] = both[:, 128:]


def pull_kernel(level, own, other, *refs):
    places = places_of([own, other])
    fronts, updates, refs = refs[:level], refs[level : level + 2], refs[level + 2 :]
    out = refs[0]
    if level == 1:
        front, base = fronts[0], 48
    else:
        front, base = refs[1], 0
        front[48:112] = fronts[0][...]
        front[16:48] = fronts[1][...]
        if level == 3:
            front[0:16] = fronts[2][...]
    total, j = None, 0
    for update in updates:
        for start in range(0, update.shape[0], 2):
            rows = jnp.concatenate(
                [front[places(j) - base], front[places(j + 1) - base]], axis=1
            )
            part = product(
                rows, update[start : start + 2].reshape(256, update.shape[2]), False
            )
            total = part if total is None else total + part
            j += 2
    for i in range(out.shape[0]):
        out[i] = total


def last_kernel(me, *refs):
    solved, pieces, kept, given = refs[:3], refs[3], refs[4], refs[5]
    for out, core in ((kept, me[0]), (given, 1 - me[0])):
        for b in range(2):
            block = core * 2 + b
            for level in range(3):
                out[level, b] = solved[level][block]
            out[3, b] = summed(pieces, block)


def merge_kernel(me, kept, given, *outs):
    mine = pl.ds(pl.multiple_of(me[0] * 16, 16), 16)
    theirs = pl.ds(pl.multiple_of((1 - me[0]) * 16, 16), 16)
    for level in range(4):
        outs[level][:, mine] = kept[level]
        outs[level][:, theirs] = given[level]


def body(*args):
    sources, inverse = args[0:4], args[4:8]
    update, links = [None, *args[8:11]], [None, *args[11:14]]
    me = lax.axis_index("core").astype(jnp.int32).reshape(1)
    widths = [i.shape[2] for i in inverse]
    rows = 16

    def pair(x):
        return [x, swapped(x, "core")]

    source_of, inverses, updates, index = ([None] * 4 for _ in range(4))
    source_of[3], inverses[3] = pair(sources[3]), pair(inverse[3])
    updates[3], index[3] = pair(update[3]), pair(links[3])
    rest = (sources[:3], inverse[:3], update[1:3], links[1:3])
    early = (source_of[3][1], inverses[3][1], updates[3][1])
    rest = lax.optimization_barrier((rest, early))[0]
    for level in (2, 1, 0):
        source_of[level], inverses[level] = pair(rest[0][level]), pair(rest[1][level])
        if level:
            updates[level], index[level] = pair(rest[2][level - 1]), pair(rest[3][level - 1])

    def value(level, lead, n):
        return call(
            functools.partial(value_kernel, bool(lead)),
            (n, rows, widths[level]),
            [me],
            [*lead, *source_of[level], *inverses[level]],
            fetch=4 if level == 3 else 0,
        )

    def push(level, lead, sizes, scratch):
        return call(
            functools.partial(push_kernel, level),
            [(rows, widths[level]), *((n, rows, 128) for n in sizes)],
            index[level],
            [*lead, *updates[level]],
            [pltpu.VMEM((112, rows, 128), F32)] if scratch else [],
            fetch=2 if level == 3 else 0,
        )

    def copied(pieces, n):
        return call(copies_kernel, (n, *pieces.shape[1:]), [], [pieces])

    def delivered(dense, level):
        pieces = exchange(dense.reshape(-1, 4, rows, 128), CHIPS[level])
        return exchange(copied(pieces, 8), ("row",))

    part3 = value(3, [], 1)[0]
    y3, dense, rest = push(3, [part3, swapped(part3, "xl")], (16, 96), True)
    dense, source_of, inverses, updates, index = lax.optimization_barrier(
        (dense, source_of, inverses, updates, index)
    )
    pieces = exchange(value(2, [delivered(dense, 2)], 4), X4)
    y2, dense, rest = push(2, [pieces, rest], (32, 64), True)
    arrived = delivered(dense, 1)
    pieces = exchange(value(1, [arrived], 8), CHIPS[1])
    y1, dense = push(1, [pieces, rest], (64,), True)
    arrived = delivered(dense, 0)
    pieces = exchange(value(0, [arrived], 4), X4)
    pieces = exchange(copied(pieces, 4), Y4)

    def row_pieces(level, minus, lead):
        out = call(
            functools.partial(solution_kernel, minus),
            (8, 4, rows, 128),
            [me],
            [*lead, *inverses[level]],
        )
        return exchange(out, ("row",))

    def shared(pieces, level):
        n = size_of(CHIPS[level])
        solved, out = call(
            share_kernel, [(4, rows, 128), (n, 4, rows, 128)], [], [pieces]
        )
        return solved, exchange(out, CHIPS[level]).reshape(-1, rows, 128)

    def pull(level, fronts, n):
        return call(
            functools.partial(pull_kernel, level),
            (n, rows, widths[level]),
            index[level],
            [*fronts, *updates[level]],
            [pltpu.VMEM((112, rows, 128), F32)] if level > 1 else [],
        )

    x0, front0 = shared(row_pieces(0, 0, [pieces]), 0)
    pieces = exchange(pull(1, [front0], 8), CHIPS[1])
    x1, front1 = shared(row_pieces(1, 1, [y1, pieces]), 1)
    pieces = exchange(pull(2, [front0, front1], 4), X4)
    x2, front2 = shared(row_pieces(2, 1, [y2, pieces]), 2)
    part3 = pull(3, [front0, front1, front2], 1)[0]
    pieces = row_pieces(3, 2, [y3, part3, swapped(part3, "xl")])
    kept, given = call(
        last_kernel, [(4, 2, rows, 128)] * 2, [me], [x0, x1, x2, pieces]
    )
    return tuple(
        call(merge_kernel, [(2, 32, 128)] * 4, [me], [kept, swapped(given, "core")])
    )


def solution(mesh):
    fine = Mesh(mesh.devices.reshape(2, 2, 2, 2, 2, 8), AXES)
    vector, matrix, index = P(LEAF, None, None), P(LEAF, None, "row"), P(LEAF)
    return jax.shard_map(
        body,
        mesh=fine,
        in_specs=(vector,) * 4 + (matrix,) * 7 + (index,) * 3,
        out_specs=(vector,) * 4,
        check_vma=False,
    )
```

```python
import functools
import math

import jax
import jax.numpy as jnp
from jax import lax
from jax.experimental import pallas as pl
from jax.experimental.pallas import tpu as pltpu
from jax.sharding import Mesh, PartitionSpec as P


AXES = ("yh", "yl", "xh", "xl", "core", "row")
LEAF = AXES[:5]
X4 = ("xh", "xl")
Y4 = ("yh", "yl")
CHIPS = [Y4 + X4, ("yl",) + X4, X4]
F32 = jnp.float32


def size_of(axes):
    total = 1
    for axis in axes:
        total *= lax.axis_size(axis)
    return total


def exchange(pieces, axes):
    return lax.all_to_all(pieces, axes, split_axis=0, concat_axis=0, tiled=True)


def swapped(x, axis):
    return lax.ppermute(x, axis, [(0, 1), (1, 0)])


def halves(x):
    high = x.astype(jnp.bfloat16)
    return high, (x - high.astype(F32)).astype(jnp.bfloat16)


def doubled(a):
    high = a.astype(jnp.bfloat16).astype(F32)
    return jnp.concatenate([high, a - high], axis=0).astype(jnp.bfloat16)


def product(rows, matrix, transposed):
    r = rows.shape[0]
    pair = doubled(rows)
    high, low = halves(matrix)
    dims = (((1,), (1 if transposed else 0,)), ((), ()))
    both = lax.dot_general(pair, high, dims, preferred_element_type=F32)
    both = both + lax.dot_general(pair, low, dims, preferred_element_type=F32)
    return both[:r] + both[r:]


def summed(ref, *index):
    total = ref[(0, *index)]
    for i in range(1, ref.shape[0]):
        total = total + ref[(i, *index)]
    return total


def call(kernel, outs, scalars, arrays, scratch=(), flops=2_000_000):
    size = sum(a.size for a in arrays) * 4
    single = isinstance(outs, tuple)
    shapes = [outs] if single else list(outs)
    size += sum(math.prod(s) for s in shapes) * 4
    room = size + sum(math.prod(s.shape) for s in scratch) * 4
    result = pl.pallas_call(
        kernel,
        out_shape=[jax.ShapeDtypeStruct(s, F32) for s in shapes],
        in_specs=[pl.BlockSpec(memory_space=pltpu.SMEM)] * len(scalars)
        + [pl.BlockSpec(memory_space=pltpu.VMEM)] * len(arrays),
        out_specs=[pl.BlockSpec(memory_space=pltpu.VMEM)] * len(shapes),
        scratch_shapes=list(scratch),
        compiler_params=pltpu.CompilerParams(vmem_limit_bytes=room + 3 * 2**20),
        cost_estimate=pl.CostEstimate(
            flops=flops, bytes_accessed=size, transcendentals=0
        ),
    )(*scalars, *arrays)
    return result[0] if single else result


def place_of(link):
    level = link >> 6
    return jnp.where(
        level == 0,
        48 + link,
        jnp.where(level == 1, 16 + (link & 31), link & 15),
    )


def places_of(refs):
    count = refs[0].shape[0]
    return lambda j: place_of(refs[j // count][j % count])


def value_kernel(arrives, me, *refs):
    refs = list(refs)
    arrived = refs.pop(0) if arrives else None
    sources, inverses, out = refs[:2], refs[2:4], refs[4]
    row = pl.multiple_of(me[0] * 16, 16)
    total = None
    for k in range(2):
        rows = []
        for b in range(2):
            w = sources[k][b, pl.ds(row, 16)]
            if arrives:
                w = w - summed(arrived, (me[0] ^ k) * 2 + b)
            rows.append(w)
        width = inverses[k].shape[2]
        part = product(
            jnp.concatenate(rows, axis=1), inverses[k][...].reshape(256, width), False
        )
        total = part if total is None else total + part
    for i in range(out.shape[0]):
        out[i] = total


def push_kernel(level, own, other, *refs):
    places = places_of([own, other])
    if level == 3:
        solved, refs = refs[0][...] + refs[1][...], refs[2:]
    else:
        solved, old, refs = summed(refs[0]), refs[1], refs[2:]
    updates, refs = refs[:2], refs[2:]
    solved_ref, dense = refs[0], refs[-1]
    solved_ref[...] = solved
    if level == 3:
        dense[...] = jnp.zeros(dense.shape, F32)
    elif level == 2:
        dense[16:112] = old[...]
    else:
        dense[48:112] = old[...]
    j = 0
    for update in updates:
        for start in range(0, update.shape[0], 2):
            both = product(
                solved, update[start : start + 2].reshape(256, update.shape[2]), True
            )
            dense[places(j)] += both[:, :128]
            dense[places(j + 1)] += both[:, 128:]
            j += 2
    if level == 3:
        refs[1][...] = dense[0:16]
        refs[2][...] = dense[16:112]
    elif level == 2:
        refs[1][...] = dense[16:48]
        refs[2][...] = dense[48:112]
    else:
        refs[1][...] = dense[48:112]


def copies_kernel(pieces, out):
    total = summed(pieces)
    for i in range(out.shape[0]):
        out[i] = total


def share_kernel(pieces, solved, out):
    total = summed(pieces)
    solved[...] = total
    for i in range(out.shape[0]):
        out[i] = total


def solution_kernel(minus, me, *refs):
    if minus == 0:
        refs, z = refs[1:], summed(refs[0])
    elif minus == 1:
        refs, z = refs[2:], refs[0][...] - summed(refs[1])
    else:
        refs, z = refs[3:], refs[0][...] - (refs[1][...] + refs[2][...])
    inverses, out = refs[:2], refs[2]
    for k in range(2):
        both = product(z, inverses[k][...].reshape(256, inverses[k].shape[2]), True)
        slot = (me[0] ^ k) * 2
        for i in range(out.shape[0]):
            out[i, slot] = both[:, :128]
            out[i, slot + 1] = both[:, 128:]


def pull_kernel(level, own, other, *refs):
    places = places_of([own, other])
    fronts, updates, refs = refs[:level], refs[level : level + 2], refs[level + 2 :]
    out = refs[0]
    if level == 1:
        front, base = fronts[0], 48
    else:
        front, base = refs[1], 0
        front[48:112] = fronts[0][...]
        front[16:48] = fronts[1][...]
        if level == 3:
            front[0:16] = fronts[2][...]
    total, j = None, 0
    for update in updates:
        for start in range(0, update.shape[0], 2):
            rows = jnp.concatenate(
                [front[places(j) - base], front[places(j + 1) - base]], axis=1
            )
            part = product(
                rows, update[start : start + 2].reshape(256, update.shape[2]), False
            )
            total = part if total is None else total + part
            j += 2
    for i in range(out.shape[0]):
        out[i] = total


def last_kernel(me, *refs):
    solved, pieces, kept, given = refs[:3], refs[3], refs[4], refs[5]
    for out, core in ((kept, me[0]), (given, 1 - me[0])):
        for b in range(2):
            block = core * 2 + b
            for level in range(3):
                out[level, b] = solved[level][block]
            out[3, b] = summed(pieces, block)


def merge_kernel(me, kept, given, *outs):
    mine = pl.ds(pl.multiple_of(me[0] * 16, 16), 16)
    theirs = pl.ds(pl.multiple_of((1 - me[0]) * 16, 16), 16)
    for level in range(4):
        outs[level][:, mine] = kept[level]
        outs[level][:, theirs] = given[level]


def body(*args):
    sources, inverse = args[0:4], args[4:8]
    update, links = [None, *args[8:11]], [None, *args[11:14]]
    me = lax.axis_index("core").astype(jnp.int32).reshape(1)
    widths = [i.shape[2] for i in inverse]
    rows = 16

    def pair(x):
        return [x, swapped(x, "core")]

    source_of, inverses, updates, index = ([None] * 4 for _ in range(4))
    source_of[3], inverses[3] = pair(sources[3]), pair(inverse[3])
    updates[3], index[3] = pair(update[3]), pair(links[3])
    index[1], index[2] = pair(links[1]), pair(links[2])

    def value(level, lead, n):
        return call(
            functools.partial(value_kernel, bool(lead)),
            (n, rows, widths[level]),
            [me],
            [*lead, *source_of[level], *inverses[level]],
        )

    def push(level, lead, sizes, scratch):
        return call(
            functools.partial(push_kernel, level),
            [(rows, widths[level]), *((n, rows, 128) for n in sizes)],
            index[level],
            [*lead, *updates[level]],
            [pltpu.VMEM((112, rows, 128), F32)] if scratch else [],
        )

    def copied(pieces, n):
        return call(copies_kernel, (n, *pieces.shape[1:]), [], [pieces])

    def delivered(dense, level):
        pieces = exchange(dense.reshape(-1, 4, rows, 128), CHIPS[level])
        return exchange(copied(pieces, 8), ("row",))

    part3 = value(3, [], 1)[0]
    part3, index, rest, _ = lax.optimization_barrier(
        (part3, index, (sources[:3], inverse[:3], update[1:3]), updates[3][1])
    )
    far3 = swapped(part3, "xl")
    for level in (2, 1, 0):
        source_of[level], inverses[level] = pair(rest[0][level]), pair(rest[1][level])
        if level:
            updates[level] = pair(rest[2][level - 1])
    y3, dense, rest = push(3, [part3, far3], (16, 96), True)
    dense, source_of, inverses, updates, index = lax.optimization_barrier(
        (dense, source_of, inverses, updates, index)
    )
    pieces = exchange(value(2, [delivered(dense, 2)], 4), X4)
    y2, dense, rest = push(2, [pieces, rest], (32, 64), True)
    arrived = delivered(dense, 1)
    pieces = exchange(value(1, [arrived], 8), CHIPS[1])
    y1, dense = push(1, [pieces, rest], (64,), True)
    arrived = delivered(dense, 0)
    pieces = exchange(value(0, [arrived], 4), X4)
    pieces = exchange(copied(pieces, 4), Y4)

    def row_pieces(level, minus, lead):
        out = call(
            functools.partial(solution_kernel, minus),
            (8, 4, rows, 128),
            [me],
            [*lead, *inverses[level]],
        )
        return exchange(out, ("row",))

    def shared(pieces, level):
        n = size_of(CHIPS[level])
        solved, out = call(
            share_kernel, [(4, rows, 128), (n, 4, rows, 128)], [], [pieces]
        )
        return solved, exchange(out, CHIPS[level]).reshape(-1, rows, 128)

    def pull(level, fronts, n):
        return call(
            functools.partial(pull_kernel, level),
            (n, rows, widths[level]),
            index[level],
            [*fronts, *updates[level]],
            [pltpu.VMEM((112, rows, 128), F32)] if level > 1 else [],
        )

    x0, front0 = shared(row_pieces(0, 0, [pieces]), 0)
    pieces = exchange(pull(1, [front0], 8), CHIPS[1])
    x1, front1 = shared(row_pieces(1, 1, [y1, pieces]), 1)
    pieces = exchange(pull(2, [front0, front1], 4), X4)
    x2, front2 = shared(row_pieces(2, 1, [y2, pieces]), 2)
    part3 = pull(3, [front0, front1, front2], 1)[0]
    pieces = row_pieces(3, 2, [y3, part3, swapped(part3, "xl")])
    kept, given = call(
        last_kernel, [(4, 2, rows, 128)] * 2, [me], [x0, x1, x2, pieces]
    )
    return tuple(
        call(merge_kernel, [(2, 32, 128)] * 4, [me], [kept, swapped(given, "core")])
    )


def solution(mesh):
    fine = Mesh(mesh.devices.reshape(2, 2, 2, 2, 2, 8), AXES)
    vector, matrix, index = P(LEAF, None, None), P(LEAF, None, "row"), P(LEAF)
    return jax.shard_map(
        body,
        mesh=fine,
        in_specs=(vector,) * 4 + (matrix,) * 7 + (index,) * 3,
        out_specs=(vector,) * 4,
        check_vma=False,
    )
```

```python
import functools
import math

import jax
import jax.numpy as jnp
from jax import lax
from jax.experimental import pallas as pl
from jax.experimental.pallas import tpu as pltpu
from jax.sharding import Mesh, PartitionSpec as P


AXES = ("yh", "yl", "xh", "xl", "core", "row")
LEAF = AXES[:5]
X4 = ("xh", "xl")
Y4 = ("yh", "yl")
CHIPS = [Y4 + X4, ("yl",) + X4, X4]
F32 = jnp.float32


def size_of(axes):
    total = 1
    for axis in axes:
        total *= lax.axis_size(axis)
    return total


def exchange(pieces, axes):
    return lax.all_to_all(pieces, axes, split_axis=0, concat_axis=0, tiled=True)


def swapped(x, axis):
    return lax.ppermute(x, axis, [(0, 1), (1, 0)])


def halves(x):
    high = x.astype(jnp.bfloat16)
    return high, (x - high.astype(F32)).astype(jnp.bfloat16)


def doubled(a):
    high = a.astype(jnp.bfloat16).astype(F32)
    return jnp.concatenate([high, a - high], axis=0).astype(jnp.bfloat16)


def product(rows, matrix, transposed):
    r = rows.shape[0]
    pair = doubled(rows)
    high, low = halves(matrix)
    dims = (((1,), (1 if transposed else 0,)), ((), ()))
    both = lax.dot_general(pair, high, dims, preferred_element_type=F32)
    both = both + lax.dot_general(pair, low, dims, preferred_element_type=F32)
    return both[:r] + both[r:]


def summed(ref, *index):
    total = ref[(0, *index)]
    for i in range(1, ref.shape[0]):
        total = total + ref[(i, *index)]
    return total


def call(kernel, outs, scalars, arrays, scratch=(), flops=2_000_000):
    size = sum(a.size for a in arrays) * 4
    single = isinstance(outs, tuple)
    shapes = [outs] if single else list(outs)
    size += sum(math.prod(s) for s in shapes) * 4
    room = size + sum(math.prod(s.shape) for s in scratch) * 4
    result = pl.pallas_call(
        kernel,
        out_shape=[jax.ShapeDtypeStruct(s, F32) for s in shapes],
        in_specs=[pl.BlockSpec(memory_space=pltpu.SMEM)] * len(scalars)
        + [pl.BlockSpec(memory_space=pltpu.VMEM)] * len(arrays),
        out_specs=[pl.BlockSpec(memory_space=pltpu.VMEM)] * len(shapes),
        scratch_shapes=list(scratch),
        compiler_params=pltpu.CompilerParams(vmem_limit_bytes=room + 3 * 2**20),
        cost_estimate=pl.CostEstimate(
            flops=flops, bytes_accessed=size, transcendentals=0
        ),
    )(*scalars, *arrays)
    return result[0] if single else result


def place_of(link):
    level = link >> 6
    return jnp.where(
        level == 0,
        48 + link,
        jnp.where(level == 1, 16 + (link & 31), link & 15),
    )


def places_of(refs):
    count = refs[0].shape[0]
    return lambda j: place_of(refs[j // count][j % count])


def value_kernel(arrives, me, *refs):
    refs = list(refs)
    arrived = refs.pop(0) if arrives else None
    sources, inverses, out = refs[:2], refs[2:4], refs[4]
    row = pl.multiple_of(me[0] * 16, 16)
    total = None
    for k in range(2):
        rows = []
        for b in range(2):
            w = sources[k][b, pl.ds(row, 16)]
            if arrives:
                w = w - summed(arrived, (me[0] ^ k) * 2 + b)
            rows.append(w)
        width = inverses[k].shape[2]
        part = product(
            jnp.concatenate(rows, axis=1), inverses[k][...].reshape(256, width), False
        )
        total = part if total is None else total + part
    for i in range(out.shape[0]):
        out[i] = total


def push_kernel(level, own, other, *refs):
    places = places_of([own, other])
    if level == 3:
        solved, refs = refs[0][...] + refs[1][...], refs[2:]
    else:
        solved, old, refs = summed(refs[0]), refs[1], refs[2:]
    updates, refs = refs[:2], refs[2:]
    solved_ref, dense = refs[0], refs[-1]
    solved_ref[...] = solved
    if level == 3:
        dense[...] = jnp.zeros(dense.shape, F32)
    elif level == 2:
        dense[16:112] = old[...]
    else:
        dense[48:112] = old[...]
    j = 0
    for update in updates:
        for start in range(0, update.shape[0], 2):
            both = product(
                solved, update[start : start + 2].reshape(256, update.shape[2]), True
            )
            dense[places(j)] += both[:, :128]
            dense[places(j + 1)] += both[:, 128:]
            j += 2
    if level == 3:
        refs[1][...] = dense[0:16]
        refs[2][...] = dense[16:112]
    elif level == 2:
        refs[1][...] = dense[16:48]
        refs[2][...] = dense[48:112]
    else:
        refs[1][...] = dense[48:112]


def copies_kernel(pieces, out):
    total = summed(pieces)
    for i in range(out.shape[0]):
        out[i] = total


def share_kernel(pieces, solved, out):
    total = summed(pieces)
    solved[...] = total
    for i in range(out.shape[0]):
        out[i] = total


def solution_kernel(minus, me, *refs):
    if minus == 0:
        refs, z = refs[1:], summed(refs[0])
    elif minus == 1:
        refs, z = refs[2:], refs[0][...] - summed(refs[1])
    else:
        refs, z = refs[3:], refs[0][...] - (refs[1][...] + refs[2][...])
    inverses, out = refs[:2], refs[2]
    for k in range(2):
        both = product(z, inverses[k][...].reshape(256, inverses[k].shape[2]), True)
        slot = (me[0] ^ k) * 2
        for i in range(out.shape[0]):
            out[i, slot] = both[:, :128]
            out[i, slot + 1] = both[:, 128:]


def pull_kernel(level, own, other, *refs):
    places = places_of([own, other])
    fronts, updates, refs = refs[:level], refs[level : level + 2], refs[level + 2 :]
    out = refs[0]
    if level == 1:
        front, base = fronts[0], 48
    else:
        front, base = refs[1], 0
        front[48:112] = fronts[0][...]
        front[16:48] = fronts[1][...]
        if level == 3:
            front[0:16] = fronts[2][...]
    total, j = None, 0
    for update in updates:
        for start in range(0, update.shape[0], 2):
            rows = jnp.concatenate(
                [front[places(j) - base], front[places(j + 1) - base]], axis=1
            )
            part = product(
                rows, update[start : start + 2].reshape(256, update.shape[2]), False
            )
            total = part if total is None else total + part
            j += 2
    for i in range(out.shape[0]):
        out[i] = total


def last_kernel(me, *refs):
    solved, pieces, kept, given = refs[:3], refs[3], refs[4], refs[5]
    for out, core in ((kept, me[0]), (given, 1 - me[0])):
        for b in range(2):
            block = core * 2 + b
            for level in range(3):
                out[level, b] = solved[level][block]
            out[3, b] = summed(pieces, block)


def merge_kernel(me, kept, given, *outs):
    mine = pl.ds(pl.multiple_of(me[0] * 16, 16), 16)
    theirs = pl.ds(pl.multiple_of((1 - me[0]) * 16, 16), 16)
    for level in range(4):
        outs[level][:, mine] = kept[level]
        outs[level][:, theirs] = given[level]


def body(*args):
    sources, inverse = args[0:4], args[4:8]
    update, links = [None, *args[8:11]], [None, *args[11:14]]
    me = lax.axis_index("core").astype(jnp.int32).reshape(1)
    widths = [i.shape[2] for i in inverse]
    rows = 16

    def pair(x):
        return [x, swapped(x, "core")]

    source_of, inverses, updates, index = ([None] * 4 for _ in range(4))
    source_of[3], inverses[3] = pair(sources[3]), pair(inverse[3])
    updates[3], index[3] = pair(update[3]), pair(links[3])
    index[1], index[2] = pair(links[1]), pair(links[2])
    for level in (2, 1, 0):
        source_of[level] = pair(sources[level])

    def value(level, lead, n):
        return call(
            functools.partial(value_kernel, bool(lead)),
            (n, rows, widths[level]),
            [me],
            [*lead, *source_of[level], *inverses[level]],
        )

    def push(level, lead, sizes, scratch):
        return call(
            functools.partial(push_kernel, level),
            [(rows, widths[level]), *((n, rows, 128) for n in sizes)],
            index[level],
            [*lead, *updates[level]],
            [pltpu.VMEM((112, rows, 128), F32)] if scratch else [],
        )

    def copied(pieces, n):
        return call(copies_kernel, (n, *pieces.shape[1:]), [], [pieces])

    def delivered(dense, level):
        pieces = exchange(dense.reshape(-1, 4, rows, 128), CHIPS[level])
        return exchange(copied(pieces, 8), ("row",))

    part3 = value(3, [], 1)[0]
    part3, index, source_of, rest, _ = lax.optimization_barrier(
        (part3, index, source_of, (inverse[:3], update[1:3]), updates[3][1])
    )
    far3 = swapped(part3, "xl")
    for level in (2, 1, 0):
        inverses[level] = pair(rest[0][level])
        if level:
            updates[level] = pair(rest[1][level - 1])
    y3, dense, rest = push(3, [part3, far3], (16, 96), True)
    dense, source_of, inverses, updates, index = lax.optimization_barrier(
        (dense, source_of, inverses, updates, index)
    )
    pieces = exchange(value(2, [delivered(dense, 2)], 4), X4)
    y2, dense, rest = push(2, [pieces, rest], (32, 64), True)
    arrived = delivered(dense, 1)
    pieces = exchange(value(1, [arrived], 8), CHIPS[1])
    y1, dense = push(1, [pieces, rest], (64,), True)
    arrived = delivered(dense, 0)
    pieces = exchange(value(0, [arrived], 4), X4)
    pieces = exchange(copied(pieces, 4), Y4)

    def row_pieces(level, minus, lead):
        out = call(
            functools.partial(solution_kernel, minus),
            (8, 4, rows, 128),
            [me],
            [*lead, *inverses[level]],
        )
        return exchange(out, ("row",))

    def shared(pieces, level):
        n = size_of(CHIPS[level])
        solved, out = call(
            share_kernel, [(4, rows, 128), (n, 4, rows, 128)], [], [pieces]
        )
        return solved, exchange(out, CHIPS[level]).reshape(-1, rows, 128)

    def pull(level, fronts, n):
        return call(
            functools.partial(pull_kernel, level),
            (n, rows, widths[level]),
            index[level],
            [*fronts, *updates[level]],
            [pltpu.VMEM((112, rows, 128), F32)] if level > 1 else [],
        )

    x0, front0 = shared(row_pieces(0, 0, [pieces]), 0)
    pieces = exchange(pull(1, [front0], 8), CHIPS[1])
    x1, front1 = shared(row_pieces(1, 1, [y1, pieces]), 1)
    pieces = exchange(pull(2, [front0, front1], 4), X4)
    x2, front2 = shared(row_pieces(2, 1, [y2, pieces]), 2)
    part3 = pull(3, [front0, front1, front2], 1)[0]
    pieces = row_pieces(3, 2, [y3, part3, swapped(part3, "xl")])
    kept, given = call(
        last_kernel, [(4, 2, rows, 128)] * 2, [me], [x0, x1, x2, pieces]
    )
    return tuple(
        call(merge_kernel, [(2, 32, 128)] * 4, [me], [kept, swapped(given, "core")])
    )


def solution(mesh):
    fine = Mesh(mesh.devices.reshape(2, 2, 2, 2, 2, 8), AXES)
    vector, matrix, index = P(LEAF, None, None), P(LEAF, None, "row"), P(LEAF)
    return jax.shard_map(
        body,
        mesh=fine,
        in_specs=(vector,) * 4 + (matrix,) * 7 + (index,) * 3,
        out_specs=(vector,) * 4,
        check_vma=False,
    )
```
